32 devices in a mesh: dp: 2 (over x), tp: 16 (over z, y, core).
Axes of the slice: x: 2, y: 2, z: 4, core: 2. Of those that a mesh axis runs over, the one named last changes fastest.
Arguments:
- x: bfloat16 [2, 4096, 2560], P('dp', 'tp'), parts along dimension 0
- ln_gain: bfloat16 [2, 2560], replicated
- ln_bias: bfloat16 [2, 2560], replicated
- w_q: bfloat16 [2, 2560, 32, 80], P(None, None, 'tp')
- b_q: bfloat16 [2, 32, 80], P(None, 'tp')
- w_k: bfloat16 [2, 2560, 32, 80], P(None, None, 'tp')
- b_k: bfloat16 [2, 32, 80], P(None, 'tp')
- w_v: bfloat16 [2, 2560, 32, 80], P(None, None, 'tp')
- b_v: bfloat16 [2, 32, 80], P(None, 'tp')
- w_o: bfloat16 [2, 32, 80, 2560], P(None, 'tp')
- b_o: bfloat16 [2, 2560], replicated
- w_up: bfloat16 [2, 2560, 10240], P(None, None, 'tp')
- b_up: bfloat16 [2, 10240], P(None, 'tp')
- w_down: bfloat16 [2, 10240, 2560], P(None, 'tp')
- b_down: bfloat16 [2, 2560], replicated
Outputs:
- output: bfloat16 [2, 4096, 2560], P('dp', 'tp'), parts along dimension 0
There are 2 independent parts. The reference program is written for one: setup_inputs(seed, part) draws one part's arguments, and reference() takes and returns one part's arrays. A program takes and returns all parts, laid end to end along the dimension named above; an argument that names none is the same for every part.
All inputs are finite; a program needn't handle non-finite values.
Results may differ from the reference program's by a relative error of at most 0.0175827.
Values are sent between devices in bfloat16 or wider.
A program may use at most 1 GiB of HBM per device.

```python
import jax
import jax.numpy as jnp
from jax import lax

N_BATCH = 1
SEQ_LEN = 4096
D_MODEL = 2560
N_HEADS = 32
HEAD_DIM = 80
D_FF = 10240
ROT_DIM = 32
N_LAYERS = 2


def setup_inputs(seed: int = 0, part: int = 0) -> dict:
    shared_keys = jax.random.split(jax.random.key(seed), 14)
    token_key = jax.random.fold_in(jax.random.key(seed + 1), part)

    def draw(key_index, shape, scale, offset):
        sample = jax.random.normal(shared_keys[key_index], shape, jnp.float32)
        return (offset + scale * sample).astype(jnp.bfloat16)

    proj_shape = (N_LAYERS, D_MODEL, N_HEADS, HEAD_DIM)
    head_shape = (N_LAYERS, N_HEADS, HEAD_DIM)
    wide_shape = (N_LAYERS, D_MODEL)
    in_scale = D_MODEL ** -0.5
    x = jax.random.normal(token_key, (N_BATCH, SEQ_LEN, D_MODEL), jnp.float32).astype(jnp.bfloat16)
    return {
        "x": x,
        "ln_gain": draw(0, wide_shape, 0.3, 1.0),
        "ln_bias": draw(1, wide_shape, 0.3, 0.0),
        "w_q": draw(2, proj_shape, 2.0 * in_scale, 0.0),
        "b_q": draw(3, head_shape, 0.5, 0.0),
        "w_k": draw(4, proj_shape, 2.0 * in_scale, 0.0),
        "b_k": draw(5, head_shape, 0.5, 0.0),
        "w_v": draw(6, proj_shape, in_scale, 0.0),
        "b_v": draw(7, head_shape, 0.5, 0.0),
        "w_o": draw(8, (N_LAYERS, N_HEADS, HEAD_DIM, D_MODEL), in_scale, 0.0),
        "b_o": draw(9, wide_shape, 0.5, 0.0),
        "w_up": draw(10, (N_LAYERS, D_MODEL, D_FF), in_scale, 0.0),
        "b_up": draw(11, (N_LAYERS, D_FF), 0.5, 0.0),
        "w_down": draw(12, (N_LAYERS, D_FF, D_MODEL), D_FF ** -0.5, 0.0),
        "b_down": draw(13, wide_shape, 0.5, 0.0),
    }


def rotary_tables():
    half = ROT_DIM // 2
    inv_freq = 1.0 / (10000.0 ** (jnp.arange(half, dtype=jnp.float32) * (2.0 / ROT_DIM)))
    angles = jnp.arange(SEQ_LEN, dtype=jnp.float32)[:, None] * inv_freq[None, :]
    return jnp.cos(angles)[:, None, :], jnp.sin(angles)[:, None, :]


def apply_rotary(projected, cosine, sine):
    half = ROT_DIM // 2
    first = projected[..., :half]
    second = projected[..., half:ROT_DIM]
    return jnp.concatenate([first * cosine - second * sine, second * cosine + first * sine, projected[..., ROT_DIM:]], axis=-1)


def attend_heads(q_rot, k_rot, values):
    def per_head(operands):
        q_one, k_one, v_one = operands
        scores = jnp.dot(q_one, jnp.transpose(k_one), preferred_element_type=jnp.float32) * (HEAD_DIM ** -0.5)
        causal = jnp.arange(SEQ_LEN)[:, None] >= jnp.arange(SEQ_LEN)[None, :]
        attn_probs = jax.nn.softmax(jnp.where(causal, scores, -1e30), axis=-1).astype(jnp.bfloat16)
        return jnp.dot(attn_probs, v_one, preferred_element_type=jnp.float32).astype(jnp.bfloat16)

    def by_head(tensor):
        return jnp.transpose(tensor, (0, 2, 1, 3)).reshape(N_BATCH * N_HEADS, SEQ_LEN, HEAD_DIM)

    head_out = lax.map(per_head, (by_head(q_rot), by_head(k_rot), by_head(values)))
    return jnp.transpose(head_out.reshape(N_BATCH, N_HEADS, SEQ_LEN, HEAD_DIM), (0, 2, 1, 3))


def layer_forward(hidden, layer_params):
    (ln_gain, ln_bias, w_q, b_q, w_k, b_k, w_v, b_v, w_o, b_o, w_up, b_up, w_down, b_down) = layer_params
    x_f32 = hidden.astype(jnp.float32)
    mean = jnp.mean(x_f32, axis=-1, keepdims=True)
    centered = x_f32 - mean
    variance = jnp.mean(centered * centered, axis=-1, keepdims=True)
    normed = (centered * lax.rsqrt(variance + 1e-5) * ln_gain.astype(jnp.float32) + ln_bias.astype(jnp.float32)).astype(jnp.bfloat16)
    flat = normed.reshape(N_BATCH * SEQ_LEN, D_MODEL)
    head_shape = (N_BATCH, SEQ_LEN, N_HEADS, HEAD_DIM)
    cosine, sine = rotary_tables()

    def project(weight, bias):
        prod = jnp.dot(flat, weight.reshape(D_MODEL, N_HEADS * HEAD_DIM), preferred_element_type=jnp.float32)
        return prod.reshape(head_shape) + bias.astype(jnp.float32)

    q_rot = apply_rotary(project(w_q, b_q), cosine, sine).astype(jnp.bfloat16)
    k_rot = apply_rotary(project(w_k, b_k), cosine, sine).astype(jnp.bfloat16)
    values = project(w_v, b_v).astype(jnp.bfloat16)
    attended = attend_heads(q_rot, k_rot, values)
    dense_out = jnp.dot(attended.reshape(N_BATCH * SEQ_LEN, D_MODEL), w_o.reshape(D_MODEL, D_MODEL), preferred_element_type=jnp.float32)
    up_act = jax.nn.gelu(jnp.dot(flat, w_up, preferred_element_type=jnp.float32) + b_up.astype(jnp.float32), approximate=True).astype(jnp.bfloat16)
    down_out = jnp.dot(up_act, w_down, preferred_element_type=jnp.float32)
    total = x_f32.reshape(N_BATCH * SEQ_LEN, D_MODEL) + dense_out + down_out + b_o.astype(jnp.float32) + b_down.astype(jnp.float32)
    return total.reshape(N_BATCH, SEQ_LEN, D_MODEL).astype(jnp.bfloat16)


def reference(x, ln_gain, ln_bias, w_q, b_q, w_k, b_k, w_v, b_v, w_o, b_o, w_up, b_up, w_down, b_down):
    stacked = (ln_gain, ln_bias, w_q, b_q, w_k, b_k, w_v, b_v, w_o, b_o, w_up, b_up, w_down, b_down)

    def layer_body(hidden, layer_params):
        return layer_forward(hidden, layer_params), None

    final = lax.scan(layer_body, x, stacked)
    return final[0]
```

```python
import functools

import jax
import jax.numpy as jnp
from jax import lax
from jax.experimental import pallas as pl
from jax.experimental.pallas import tpu as pltpu
from jax.sharding import PartitionSpec as P

ROT_DIM = 32
ROPE_BASE = 10000.0
LN_EPS = 1e-5
LANES = 128
RING = 8
LOG2_E = 1.4426950408889634
MESH = pl.DeviceIdType.MESH
VMEM_LIMIT = 62 * 1024 * 1024
F32 = jnp.float32
BF16 = jnp.bfloat16


def ring_to_chip(pos):
    y = ((pos + 3) // 4) % 2
    z = y * (pos - 1) + (1 - y) * ((RING - pos) % RING)
    return 2 * z + y


def chip_to_ring(chip):
    y = chip % 2
    z = chip // 2
    return y * (z + 1) + (1 - y) * ((RING - z) % RING)


def place():
    me = lax.axis_index("tp")
    core = me % 2
    chip = me // 2
    pos = chip_to_ring(chip)
    right = 2 * ring_to_chip((pos + 1) % RING) + core
    left = 2 * ring_to_chip((pos + RING - 1) % RING) + core
    partner = 2 * chip + (1 - core)
    return core, chip, pos, right, left, partner


def meet(right, left, partner):
    barrier = pltpu.get_barrier_semaphore()
    for other in (right, left, partner):
        pl.semaphore_signal(barrier, inc=1, device_id={"tp": other}, device_id_type=MESH)
    pl.semaphore_wait(barrier, 3)


def layer_norm(hidden, gain, bias):
    x_f32 = hidden.astype(F32)
    mean = jnp.mean(x_f32, axis=-1, keepdims=True)
    centered = x_f32 - mean
    variance = jnp.mean(centered * centered, axis=-1, keepdims=True)
    return (centered * lax.rsqrt(variance + LN_EPS) * gain.astype(F32) + bias.astype(F32)).astype(BF16)


def gather_kernel(h_hbm, w_qkv, w_up, b_qkv, b_up, cos_t, sin_t, q_out, k_out, v_out, m_out,
                  hbuf, local_sem, ring_send, ring_recv, pair_send, pair_recv):
    half = hbuf.shape[2] // 2
    piece = half // 2
    core, chip, pos, right, left, partner = place()
    meet(right, left, partner)

    def block(way, step):
        return ring_to_chip((pos + (RING - step if way == 0 else step)) % RING)

    def rows_of(way, step, part, side):
        return hbuf.at[way, block(way, step), pl.ds(side * half + part * piece, piece)]

    def ring_copy(way, step, part):
        ref = rows_of(way, step, part, core)
        return pltpu.make_async_remote_copy(
            src_ref=ref, dst_ref=ref, send_sem=ring_send.at[way, step, part], recv_sem=ring_recv.at[way, step, part],
            device_id={"tp": right if way == 0 else left}, device_id_type=MESH)

    def ring_arrival(way, step, part):
        ref = rows_of(way, step, part, core)
        return pltpu.make_async_remote_copy(
            src_ref=ref, dst_ref=ref, send_sem=ring_send.at[way, step - 1, part], recv_sem=ring_recv.at[way, step - 1, part],
            device_id={"tp": right if way == 0 else left}, device_id_type=MESH)

    def pair_copy(way, step, part, side):
        ref = rows_of(way, step, part, side)
        return pltpu.make_async_remote_copy(
            src_ref=ref, dst_ref=ref, send_sem=pair_send.at[way, step, part], recv_sem=pair_recv.at[way, step, part],
            device_id={"tp": partner}, device_id_type=MESH)

    def own_copy(way):
        return pltpu.make_async_copy(h_hbm.at[pl.ds(way * half, half)],
                                     hbuf.at[way, chip, pl.ds(core * half, half)], local_sem.at[way])

    for way in range(2):
        own_copy(way).start()
    for way in range(2):
        own_copy(way).wait()
        for part in range(2):
            ring_copy(way, 0, part).start()
            pair_copy(way, 0, part, core).start()

    def rotate(value, cosine, sine):
        lane = lax.broadcasted_iota(jnp.int32, value.shape, 1)
        swapped = jnp.where(lane < ROT_DIM // 2, pltpu.roll(value, LANES - ROT_DIM // 2, 1), pltpu.roll(value, ROT_DIM // 2, 1))
        return value * cosine + swapped * sine

    def compute(way, step):
        for part in range(2):
            pair_copy(way, step, part, 1 - core).wait_recv()
        at = block(way, step)
        normed = hbuf[way, at]
        cosine, sine = cos_t[at, way], sin_t[at, way]
        width = w_qkv.shape[1] // 3
        for which, out in enumerate((q_out, k_out, v_out)):
            cols = slice(which * width, (which + 1) * width)
            proj = jnp.dot(normed, w_qkv[:, cols], preferred_element_type=F32) + b_qkv[:, cols]
            if which < 2:
                for head in range(width // LANES):
                    lanes = slice(head * LANES, (head + 1) * LANES)
                    out[at, way, :, lanes] = rotate(proj[:, lanes], cosine, sine).astype(BF16)
            else:
                out[at, way] = proj.astype(BF16)
        up = jnp.dot(normed, w_up[...], preferred_element_type=F32) + b_up[...]
        m_out[at, way] = jax.nn.gelu(up, approximate=True).astype(BF16)

    def step_body(step, carry):
        for part in range(2):
            for way in range(2):
                ring_arrival(way, step, part).wait_recv()

                @pl.when(step < RING - 1)
                def _():
                    ring_copy(way, step, part).start()

                pair_copy(way, step, part, core).start()
            compute(part, step - 1)
        return carry

    lax.fori_loop(1, RING, step_body, 0)
    for way in range(2):
        compute(way, RING - 1)

    def drain(step, carry):
        for way in range(2):
            for part in range(2):
                @pl.when(step < RING - 1)
                def _():
                    ring_copy(way, step, part).wait_send()

                pair_copy(way, step, part, core).wait_send()
        return carry

    lax.fori_loop(0, RING, drain, 0)


def gather_project(h, w_qkv, w_up, b_qkv, b_up, cos_t, sin_t, collective_id):
    rows, depth = h.shape
    qkv_shape = jax.ShapeDtypeStruct((RING, 2, rows, w_qkv.shape[1] // 3), BF16)
    m_shape = jax.ShapeDtypeStruct((RING, 2, rows, w_up.shape[1]), BF16)
    vmem = pl.BlockSpec(memory_space=pltpu.VMEM)
    return pl.pallas_call(
        gather_kernel,
        out_shape=(qkv_shape, qkv_shape, qkv_shape, m_shape),
        in_specs=[pl.BlockSpec(memory_space=pl.ANY)] + [vmem] * 6,
        out_specs=(vmem,) * 4,
        scratch_shapes=[
            pltpu.VMEM((2, RING, rows, depth), BF16),
            pltpu.SemaphoreType.DMA((2,)),
            pltpu.SemaphoreType.DMA((2, RING, 2)),
            pltpu.SemaphoreType.DMA((2, RING, 2)),
            pltpu.SemaphoreType.DMA((2, RING, 2)),
            pltpu.SemaphoreType.DMA((2, RING, 2)),
        ],
        compiler_params=pltpu.CompilerParams(collective_id=collective_id, has_side_effects=True, vmem_limit_bytes=VMEM_LIMIT),
        name=f"gather_project_{collective_id}",
    )(h, w_qkv, w_up, b_qkv, b_up, cos_t, sin_t)


def scatter_kernel(last, head_dim, q_ref, k_ref, v_ref, m_ref, w_o, w_down, x_ref, b_o, b_down, gain, bias, *refs):
    if last:
        hid_out, h_out = refs[0], None
        refs = refs[1:]
    else:
        hid_out, h_out = refs[0], refs[1]
        refs = refs[2:]
    acc, top, held, given, taken, own, ring_send, ring_recv, pair_send, pair_recv = refs
    rows = q_ref.shape[2]
    half = rows // 2
    piece = half // 2
    depth = w_o.shape[1]
    heads = q_ref.shape[3] // LANES
    tile = next(t for t in (512, 256, 128) if depth % t == 0)
    scale = head_dim ** -0.5 * LOG2_E
    core, chip, pos, right, left, partner = place()
    mine, other = pl.ds(core * half, half), pl.ds((1 - core) * half, half)

    for way in range(2):
        held[way, 0] = jnp.zeros((half, depth), BF16)
    meet(right, left, partner)

    def block(way, step):
        return ring_to_chip((pos + (2 * RING - 1 - step if way == 0 else 1 + step)) % RING)

    def ring_copy(way, step, part):
        span = pl.ds(part * piece, piece)
        return pltpu.make_async_remote_copy(
            src_ref=held.at[way, step, span], dst_ref=held.at[way, step + 1, span],
            send_sem=ring_send.at[way, step, part], recv_sem=ring_recv.at[way, step, part],
            device_id={"tp": right if way == 0 else left}, device_id_type=MESH)

    def pair_copy(way, step):
        return pltpu.make_async_remote_copy(
            src_ref=given.at[way, step % 2], dst_ref=taken.at[way, step],
            send_sem=pair_send.at[way, step], recv_sem=pair_recv.at[way, step],
            device_id={"tp": partner}, device_id_type=MESH)

    def attend(way, at):
        row = lax.broadcasted_iota(jnp.int32, (rows, 1), 0)
        row_side = (row // half + core) % 2
        row_pos = row_side * (2 * half) + way * half + row % half
        col = lax.broadcasted_iota(jnp.int32, (1, 2 * rows), 1)
        col_pos = ((col // half) % 2) * (2 * half) + (col // rows) * half + col % half
        queries = []
        for head in range(heads):
            lanes = slice(head * LANES, (head + 1) * LANES)
            queries.append(jnp.concatenate([q_ref[at, way, mine, lanes], q_ref[at, way, other, lanes]], axis=0))
            keys = k_ref[at, :, :, lanes].reshape(2 * rows, LANES)
            values = v_ref[at, :, :, lanes].reshape(2 * rows, LANES)
            score = lax.dot_general(queries[head], keys, (((1,), (1,)), ((), ())), preferred_element_type=F32) * scale
            score = jnp.where(row_pos >= col_pos, score, -1e30)
            peak = jnp.max(score, axis=1, keepdims=True)
            prob = jnp.exp2(score - peak).astype(BF16)
            acc[head] = jnp.dot(prob, values, preferred_element_type=F32)
            top[head] = jnp.broadcast_to(peak, (rows, LANES))

        def body(earlier, carry):
            for head in range(heads):
                lanes = slice(head * LANES, (head + 1) * LANES)
                keys = k_ref[earlier, :, :, lanes].reshape(2 * rows, LANES)
                values = v_ref[earlier, :, :, lanes].reshape(2 * rows, LANES)
                score = lax.dot_general(queries[head], keys, (((1,), (1,)), ((), ())), preferred_element_type=F32) * scale
                before = top[head][:, :1]
                peak = jnp.maximum(before, jnp.max(score, axis=1, keepdims=True))
                prob = jnp.exp2(score - peak).astype(BF16)
                acc[head] = acc[head] * jnp.exp2(before - peak) + jnp.dot(prob, values, preferred_element_type=F32)
                top[head] = jnp.broadcast_to(peak, (rows, LANES))
            return carry

        lax.fori_loop(0, at, body, 0)
        done = [(acc[head] / acc[head][:, head_dim:head_dim + 1]).astype(BF16) for head in range(heads)]
        return jnp.concatenate(done, axis=1)

    def compute(way, step):
        at = block(way, step)
        attended = attend(way, at)
        up = jnp.concatenate([m_ref[at, way, mine], m_ref[at, way, other]], axis=0)

        @pl.when(step >= 2)
        def _():
            pair_copy(way, step - 2).wait_send()

        for low in range(0, depth, tile):
            cols = slice(low, low + tile)
            part_sum = (jnp.dot(attended, w_o[:, cols], preferred_element_type=F32)
                        + jnp.dot(up, w_down[:, cols], preferred_element_type=F32))
            own[way, step % 2, :, cols] = part_sum[:half]
            given[way, step % 2, :, cols] = part_sum[half:].astype(BF16)
        pair_copy(way, step).start()

    def total(way, step, part):
        span = pl.ds(part * piece, piece)
        return (own[way, step % 2, span] + taken[way, step, span].astype(F32) + held[way, step, span].astype(F32))

    for way in range(2):
        compute(way, 0)

    def step_body(step, carry):
        for part in range(2):
            for way in range(2):
                if part == 0:
                    pair_copy(way, step).wait_recv()

                @pl.when(step > 0)
                def _():
                    ring_copy(way, step - 1, part).wait_recv()

                held[way, step, pl.ds(part * piece, piece)] = total(way, step, part).astype(BF16)
                ring_copy(way, step, part).start()
            compute(part, step + 1)
        return carry

    lax.fori_loop(0, RING - 1, step_body, 0)
    for part in range(2):
        for way in range(2):
            if part == 0:
                pair_copy(way, RING - 1).wait_recv()
            ring_copy(way, RING - 2, part).wait_recv()
            span = pl.ds(way * half + part * piece, piece)
            hidden = (x_ref[span].astype(F32) + total(way, RING - 1, part) + b_o[...] + b_down[...]).astype(BF16)
            hid_out[span] = hidden
            if h_out is not None:
                h_out[span] = layer_norm(hidden, gain[...], bias[...])

    def drain(step, carry):
        for way in range(2):
            for part in range(2):
                ring_copy(way, step, part).wait_send()
        return carry

    lax.fori_loop(0, RING - 1, drain, 0)
    for way in range(2):
        for step in (RING - 2, RING - 1):
            pair_copy(way, step).wait_send()


def attend_scatter(q, k, v, m, w_o, w_down, x, b_o, b_down, gain, bias, head_dim, last, collective_id):
    rows, depth = x.shape
    half = rows // 2
    heads = q.shape[3] // LANES
    shape = jax.ShapeDtypeStruct((rows, depth), BF16)
    vmem = pl.BlockSpec(memory_space=pltpu.VMEM)
    outs = 1 if last else 2
    return pl.pallas_call(
        functools.partial(scatter_kernel, last, head_dim),
        out_shape=(shape,) * outs,
        in_specs=[vmem] * 11,
        out_specs=(vmem,) * outs,
        scratch_shapes=[
            pltpu.VMEM((heads, rows, LANES), F32),
            pltpu.VMEM((heads, rows, LANES), F32),
            pltpu.VMEM((2, RING, half, depth), BF16),
            pltpu.VMEM((2, 2, half, depth), BF16),
            pltpu.VMEM((2, RING, half, depth), BF16),
            pltpu.VMEM((2, 2, half, depth), F32),
            pltpu.SemaphoreType.DMA((2, RING, 2)),
            pltpu.SemaphoreType.DMA((2, RING, 2)),
            pltpu.SemaphoreType.DMA((2, RING)),
            pltpu.SemaphoreType.DMA((2, RING)),
        ],
        compiler_params=pltpu.CompilerParams(collective_id=collective_id, has_side_effects=True, vmem_limit_bytes=VMEM_LIMIT),
        name=f"attend_scatter_{collective_id}",
    )(q, k, v, m, w_o, w_down, x, b_o, b_down, gain, bias)


def rotary_tables(rows):
    half = rows // 2
    chip, way, core, row = jnp.meshgrid(jnp.arange(RING), jnp.arange(2), jnp.arange(2), jnp.arange(half), indexing="ij")
    position = (chip * (2 * rows) + core * rows + way * half + row).astype(F32).reshape(RING, 2, rows, 1)
    pairs = ROT_DIM // 2
    inv_freq = 1.0 / (ROPE_BASE ** (jnp.arange(pairs, dtype=F32) * (2.0 / ROT_DIM)))
    angles = position * inv_freq
    cosine, sine = jnp.cos(angles), jnp.sin(angles)
    rest = (RING, 2, rows, LANES - ROT_DIM)
    return (jnp.concatenate([cosine, cosine, jnp.ones(rest, F32)], axis=-1),
            jnp.concatenate([-sine, sine, jnp.zeros(rest, F32)], axis=-1))


def solution(mesh):
    head_spec = P(None, None, "tp", None)
    head_bias_spec = P(None, "tp", None)
    in_specs = (P("dp", "tp", None), P(), P(), head_spec, head_bias_spec, head_spec, head_bias_spec, head_spec, head_bias_spec,
                P(None, "tp", None, None), P(), P(None, None, "tp"), P(None, "tp"), P(None, "tp", None), P())

    def local_program(x_loc, ln_gain, ln_bias, w_q, b_q, w_k, b_k, w_v, b_v, w_o, b_o, w_up, b_up, w_down, b_down):
        hidden = x_loc[0]
        rows, depth = hidden.shape
        layers, _, heads, head_dim = w_q.shape
        spare = LANES - head_dim
        cos_t, sin_t = rotary_tables(rows)

        def pad_in(weight):
            return jnp.pad(weight, ((0, 0), (0, 0), (0, spare))).reshape(depth, heads * LANES)

        def pad_bias(vector, one):
            padded = jnp.pad(vector.astype(F32), ((0, 0), (0, spare)))
            if one:
                padded = padded.at[:, head_dim].set(1.0)
            return padded.reshape(1, heads * LANES)

        def row(vector):
            return vector.astype(F32).reshape(1, -1)

        normed = layer_norm(hidden, ln_gain[0], ln_bias[0])
        for layer in range(layers):
            last = layer == layers - 1
            w_qkv = jnp.concatenate([pad_in(w_q[layer]), pad_in(w_k[layer]), pad_in(w_v[layer])], axis=1)
            b_qkv = jnp.concatenate([pad_bias(b_q[layer], False), pad_bias(b_k[layer], False), pad_bias(b_v[layer], True)], axis=1)
            w_out = jnp.pad(w_o[layer], ((0, 0), (0, spare), (0, 0))).reshape(heads * LANES, depth)
            q, k, v, m = gather_project(normed, w_qkv, w_up[layer], b_qkv, row(b_up[layer]), cos_t, sin_t, 2 * layer)
            after = 0 if last else layer + 1
            results = attend_scatter(q, k, v, m, w_out, w_down[layer], hidden, row(b_o[layer]), row(b_down[layer]),
                                     row(ln_gain[after]), row(ln_bias[after]), head_dim, last, 2 * layer + 1)
            hidden = results[0]
            normed = None if last else results[1]
        return hidden[None]

    return jax.shard_map(local_program, mesh=mesh, in_specs=in_specs, out_specs=P("dp", "tp", None), check_vma=False)
```

```python
import functools

import jax
import jax.numpy as jnp
from jax import lax
from jax.experimental import pallas as pl
from jax.experimental.pallas import tpu as pltpu
from jax.sharding import PartitionSpec as P

ROT_DIM = 32
ROPE_BASE = 10000.0
LN_EPS = 1e-5
LANES = 128
RING = 8
LOG2_E = 1.4426950408889634
MESH = pl.DeviceIdType.MESH
VMEM_LIMIT = 67043328
F32 = jnp.float32
BF16 = jnp.bfloat16


def ring_to_chip(pos):
    y = ((pos + 3) // 4) % 2
    z = y * (pos - 1) + (1 - y) * ((RING - pos) % RING)
    return 2 * z + y


def chip_to_ring(chip):
    y = chip % 2
    z = chip // 2
    return y * (z + 1) + (1 - y) * ((RING - z) % RING)


def place():
    me = lax.axis_index("tp")
    core = me % 2
    chip = me // 2
    pos = chip_to_ring(chip)
    right = 2 * ring_to_chip((pos + 1) % RING) + core
    left = 2 * ring_to_chip((pos + RING - 1) % RING) + core
    partner = 2 * chip + (1 - core)
    return core, chip, pos, right, left, partner


def meet(right, left, partner):
    barrier = pltpu.get_barrier_semaphore()
    for other in (right, left, partner):
        pl.semaphore_signal(barrier, inc=1, device_id={"tp": other}, device_id_type=MESH)
    pl.semaphore_wait(barrier, 3)


def layer_norm(hidden, gain, bias):
    x_f32 = hidden.astype(F32)
    mean = jnp.mean(x_f32, axis=-1, keepdims=True)
    centered = x_f32 - mean
    variance = jnp.mean(centered * centered, axis=-1, keepdims=True)
    return (centered * lax.rsqrt(variance + LN_EPS) * gain + bias).astype(BF16)


def layers_kernel(x_ref, wq_hbm, wk_hbm, wv_hbm, wo_hbm, wup_hbm, wdown_hbm, b_qkv, b_up, b_sum, gain, bias,
                  base_cos, base_sin, step_cos, step_sin, out_ref,
                  hbuf, q_all, k_all, v_all, m_all, staged, w_qkv, w_up, w_o, w_down, given, own, acc, top,
                  weight_sem, gather_send, gather_recv, share_send, share_recv,
                  scatter_send, scatter_recv, pair_send, pair_recv, ready):
    layers, heads, head_dim, depth = wq_hbm.shape
    rows = x_ref.shape[0]
    half = rows // 2
    piece = half // 2
    width = heads * LANES
    tile = next(t for t in (512, 256, 128) if depth % t == 0)
    scale = head_dim ** -0.5 * LOG2_E
    core, chip, pos, right, left, partner = place()
    mine, other = pl.ds(pl.multiple_of(core * half, half), half), pl.ds(pl.multiple_of((1 - core) * half, half), half)

    def span_of(part):
        return pl.ds(pl.multiple_of(part * piece, piece), piece)

    def remote(src, dst, send_sem, recv_sem, to):
        return pltpu.make_async_remote_copy(src_ref=src, dst_ref=dst, send_sem=send_sem, recv_sem=recv_sem,
                                            device_id={"tp": to}, device_id_type=MESH)

    def next_of(way):
        return right if way == 0 else left

    def in_copies(layer):
        copies = [pltpu.make_async_copy(hbm.at[layer, head], staged.at[which * heads + head, pl.ds(0, head_dim)],
                                        weight_sem.at[which * heads + head])
                  for which, hbm in enumerate((wq_hbm, wk_hbm, wv_hbm)) for head in range(heads)]
        return copies + [pltpu.make_async_copy(wup_hbm.at[layer], w_up, weight_sem.at[3 * heads])]

    def out_copies(layer):
        copies = [pltpu.make_async_copy(wo_hbm.at[layer, head], w_o.at[pl.ds(head * LANES, head_dim)],
                                        weight_sem.at[3 * heads + 1 + head]) for head in range(heads)]
        return copies + [pltpu.make_async_copy(wdown_hbm.at[layer], w_down, weight_sem.at[4 * heads + 1])]

    def gathered_block(way, step):
        return ring_to_chip((pos + (1 - way) * (RING - step) + way * step) % RING)

    def gather_copy(way, step, sem_step, part):
        ref = hbuf.at[way, gathered_block(way, step), pl.ds(pl.multiple_of(core * half + part * piece, piece), piece)]
        return remote(ref, ref, gather_send.at[way, sem_step, part], gather_recv.at[way, sem_step, part], next_of(way))

    def share_copy(way, step, part, side):
        ref = hbuf.at[way, gathered_block(way, step), pl.ds(pl.multiple_of(side * half + part * piece, piece), piece)]
        return remote(ref, ref, share_send.at[way, step, part], share_recv.at[way, step, part], partner)

    def rotate(value, cosine, sine):
        lane = lax.broadcasted_iota(jnp.int32, value.shape, 1)
        swapped = jnp.where(lane < ROT_DIM // 2, pltpu.roll(value, LANES - ROT_DIM // 2, 1), pltpu.roll(value, ROT_DIM // 2, 1))
        return value * cosine + swapped * sine

    def project(layer, way, step):
        for part in range(2):
            share_copy(way, step, part, 1 - core).wait_recv()
        at = gathered_block(way, step)
        normed = hbuf[way, at]
        cos_0, sin_0, cos_1, sin_1 = base_cos[at], base_sin[at], step_cos[way], step_sin[way]
        lane = lax.broadcasted_iota(jnp.int32, (1, LANES), 1)
        sign = jnp.where(lane < ROT_DIM // 2, -1.0, 1.0)
        cosine = cos_0 * cos_1 - sin_0 * sin_1
        sine = (sin_0 * cos_1 + cos_0 * sin_1) * sign
        for which, out in enumerate((q_all, k_all, v_all)):
            cols = slice(which * width, (which + 1) * width)
            proj = jnp.dot(normed, w_qkv[:, cols], preferred_element_type=F32) + b_qkv[layer, :, cols]
            if which < 2:
                for head in range(heads):
                    lanes = slice(head * LANES, (head + 1) * LANES)
                    out[at, way, :, lanes] = rotate(proj[:, lanes], cosine, sine).astype(BF16)
            else:
                out[at, way] = proj.astype(BF16)
        up = jnp.dot(normed, w_up[...], preferred_element_type=F32) + b_up[layer]
        m_all[at, way] = jax.nn.gelu(up, approximate=True).astype(BF16)

    def scattered_block(way, step):
        return ring_to_chip((pos + (1 - way) * (2 * RING - 1 - step) + way * (1 + step)) % RING)

    def scatter_copy(way, step, part):
        span = span_of(part)
        return remote(hbuf.at[way, step, span], hbuf.at[way, step + 1, span],
                      scatter_send.at[way, step, part], scatter_recv.at[way, step, part], next_of(way))

    def pair_copy(way, step):
        return remote(given.at[way, step % 2], hbuf.at[way, step, pl.ds(half, half)],
                      pair_send.at[way, step], pair_recv.at[way, step], partner)

    def attend(way, at):
        row = lax.broadcasted_iota(jnp.int32, (rows, 1), 0)
        row_side = (row // half + core) % 2
        row_pos = row_side * (2 * half) + way * half + row % half
        col = lax.broadcasted_iota(jnp.int32, (1, 2 * rows), 1)
        col_pos = ((col // half) % 2) * (2 * half) + (col // rows) * half + col % half
        queries = []
        for head in range(heads):
            lanes = slice(head * LANES, (head + 1) * LANES)
            queries.append(jnp.concatenate([q_all[at, way, mine, lanes], q_all[at, way, other, lanes]], axis=0))
            keys = k_all[at, :, :, lanes].reshape(2 * rows, LANES)
            values = v_all[at, :, :, lanes].reshape(2 * rows, LANES)
            score = lax.dot_general(queries[head], keys, (((1,), (1,)), ((), ())), preferred_element_type=F32) * scale
            score = jnp.where(row_pos >= col_pos, score, -1e30)
            peak = jnp.max(score, axis=1, keepdims=True)
            prob = jnp.exp2(score - peak).astype(BF16)
            acc[head] = jnp.dot(prob, values, preferred_element_type=F32)
            top[head] = jnp.broadcast_to(peak, (rows, LANES))

        def body(earlier, carry):
            for head in range(heads):
                lanes = slice(head * LANES, (head + 1) * LANES)
                keys = k_all[earlier, :, :, lanes].reshape(2 * rows, LANES)
                values = v_all[earlier, :, :, lanes].reshape(2 * rows, LANES)
                score = lax.dot_general(queries[head], keys, (((1,), (1,)), ((), ())), preferred_element_type=F32) * scale
                before = top[head][:, :1]
                peak = jnp.maximum(before, jnp.max(score, axis=1, keepdims=True))
                prob = jnp.exp2(score - peak).astype(BF16)
                acc[head] = acc[head] * jnp.exp2(before - peak) + jnp.dot(prob, values, preferred_element_type=F32)
                top[head] = jnp.broadcast_to(peak, (rows, LANES))
            return carry

        lax.fori_loop(0, at, body, 0)
        done = [(acc[head] / acc[head][:, head_dim:head_dim + 1]).astype(BF16) for head in range(heads)]
        return jnp.concatenate(done, axis=1)

    def contribute(way, step, before_send):
        at = scattered_block(way, step)
        attended = attend(way, at)
        up = jnp.concatenate([m_all[at, way, mine], m_all[at, way, other]], axis=0)

        @pl.when(step >= 2)
        def _():
            pair_copy(way, step - 2).wait_send()

        for low in range(0, depth, tile):
            cols = slice(low, low + tile)
            part_sum = (jnp.dot(attended, w_o[:, cols], preferred_element_type=F32)
                        + jnp.dot(up, w_down[:, cols], preferred_element_type=F32))
            own[way, step % 2, :, cols] = part_sum[:half]
            given[way, step % 2, :, cols] = part_sum[half:].astype(BF16)
        before_send()
        pair_copy(way, step).start()

    def total(way, step, part):
        span = span_of(part)
        taken = pl.ds(pl.multiple_of(half + part * piece, piece), piece)
        return own[way, step % 2, span] + hbuf[way, step, taken].astype(F32) + hbuf[way, step, span].astype(F32)

    def tell(phase):
        for to in (right, left, partner):
            pl.semaphore_signal(ready.at[phase], inc=1, device_id={"tp": to}, device_id_type=MESH)

    for copy in in_copies(0):
        copy.start()
    for g in range(3 * heads):
        staged[g, head_dim:] = jnp.zeros((LANES - head_dim, depth), BF16)
    for head in range(heads):
        w_o[head * LANES + head_dim:(head + 1) * LANES] = jnp.zeros((LANES - head_dim, depth), BF16)
    out_ref[...] = x_ref[...]
    meet(right, left, partner)

    def layer_body(layer, carry):
        for copy in out_copies(layer):
            copy.start()
        for way in range(2):
            for part in range(2):
                low = way * half + part * piece
                hbuf[way, chip, pl.ds(pl.multiple_of(core * half + part * piece, piece), piece)] = layer_norm(
                    out_ref[low:low + piece], gain[layer], bias[layer])

        @pl.when(layer > 0)
        def _():
            pl.semaphore_wait(ready.at[2 * layer - 1], 3)

        for part in range(2):
            for way in range(2):
                gather_copy(way, 0, 0, part).start()
                share_copy(way, 0, part, core).start()

        for copy in in_copies(layer):
            copy.wait()
        for g in range(3 * heads):
            w_qkv[:, g * LANES:(g + 1) * LANES] = staged[g].T

        def arrive(event):
            step, part = 1 + event // 2, event % 2
            for way in range(2):
                gather_copy(way, step, step - 1, part).wait_recv()

                @pl.when(step < RING - 1)
                def _():
                    gather_copy(way, step, step, part).start()

                share_copy(way, step, part, core).start()

        def first_units(unit, carry):
            project(layer, unit, 0)
            return carry

        def events(event, carry):
            arrive(event)
            project(layer, (event + 1) % 2, (event + 1) // 2)
            return carry

        lax.fori_loop(0, 2, first_units, 0)
        arrive(0)
        lax.fori_loop(1, 2 * RING - 2, events, 0)
        project(layer, 1, RING - 1)

        def drain_gather(step, carry):
            for way in range(2):
                for part in range(2):
                    @pl.when(step < RING - 1)
                    def _():
                        gather_copy(way, step, step, part).wait_send()

                    share_copy(way, step, part, core).wait_send()
            return carry

        lax.fori_loop(0, RING, drain_gather, 0)
        tell(2 * layer)

        @pl.when(layer < layers - 1)
        def _():
            for copy in in_copies(layer + 1):
                copy.start()

        for copy in out_copies(layer):
            copy.wait()
        for way in range(2):
            hbuf[way, 0, :half] = jnp.zeros((half, depth), BF16)

        def first_parts(way, carry):
            def before_send():
                @pl.when(way == 0)
                def _():
                    pl.semaphore_wait(ready.at[2 * layer], 3)

            contribute(way, 0, before_send)
            return carry

        def scatter_events(event, carry):
            step, part = event // 2, event % 2
            for way in range(2):
                @pl.when(part == 0)
                def _():
                    pair_copy(way, step).wait_recv()

                @pl.when(step > 0)
                def _():
                    scatter_copy(way, step - 1, part).wait_recv()

                hbuf[way, step, span_of(part)] = total(way, step, part).astype(BF16)
                scatter_copy(way, step, part).start()
            contribute(part, step + 1, lambda: None)
            return carry

        lax.fori_loop(0, 2, first_parts, 0)
        lax.fori_loop(0, 2 * RING - 2, scatter_events, 0)
        for part in range(2):
            for way in range(2):
                if part == 0:
                    pair_copy(way, RING - 1).wait_recv()
                scatter_copy(way, RING - 2, part).wait_recv()
                low = way * half + part * piece
                hidden = out_ref[low:low + piece].astype(F32) + total(way, RING - 1, part) + b_sum[layer]
                out_ref[low:low + piece] = hidden.astype(BF16)

        def drain_scatter(step, carry):
            for way in range(2):
                for part in range(2):
                    scatter_copy(way, step, part).wait_send()
            return carry

        lax.fori_loop(0, RING - 1, drain_scatter, 0)
        for way in range(2):
            for step in (RING - 2, RING - 1):
                pair_copy(way, step).wait_send()

        @pl.when(layer < layers - 1)
        def _():
            tell(2 * layer + 1)

        return carry

    lax.fori_loop(0, layers, layer_body, 0)


def run_layers(x, w_q, w_k, w_v, w_o, w_up, w_down, b_qkv, b_up, b_sum, gain, bias, tables):
    rows, depth = x.shape
    layers, heads, head_dim, _ = w_q.shape
    width, hidden_width = heads * LANES, w_up.shape[2]
    half = rows // 2
    vmem = pl.BlockSpec(memory_space=pltpu.VMEM)
    hbm = pl.BlockSpec(memory_space=pl.ANY)
    return pl.pallas_call(
        layers_kernel,
        out_shape=jax.ShapeDtypeStruct((rows, depth), BF16),
        in_specs=[vmem] + [hbm] * 6 + [vmem] * 9,
        out_specs=vmem,
        scratch_shapes=[
            pltpu.VMEM((2, RING, rows, depth), BF16),
            pltpu.VMEM((RING, 2, rows, width), BF16),
            pltpu.VMEM((RING, 2, rows, width), BF16),
            pltpu.VMEM((RING, 2, rows, width), BF16),
            pltpu.VMEM((RING, 2, rows, hidden_width), BF16),
            pltpu.VMEM((3 * heads, LANES, depth), BF16),
            pltpu.VMEM((depth, 3 * width), BF16),
            pltpu.VMEM((depth, hidden_width), BF16),
            pltpu.VMEM((width, depth), BF16),
            pltpu.VMEM((hidden_width, depth), BF16),
            pltpu.VMEM((2, 2, half, depth), BF16),
            pltpu.VMEM((2, 2, half, depth), F32),
            pltpu.VMEM((heads, rows, LANES), F32),
            pltpu.VMEM((heads, rows, LANES), F32),
            pltpu.SemaphoreType.DMA((4 * heads + 2,)),
            pltpu.SemaphoreType.DMA((2, RING, 2)),
            pltpu.SemaphoreType.DMA((2, RING, 2)),
            pltpu.SemaphoreType.DMA((2, RING, 2)),
            pltpu.SemaphoreType.DMA((2, RING, 2)),
            pltpu.SemaphoreType.DMA((2, RING, 2)),
            pltpu.SemaphoreType.DMA((2, RING, 2)),
            pltpu.SemaphoreType.DMA((2, RING)),
            pltpu.SemaphoreType.DMA((2, RING)),
            pltpu.SemaphoreType.REGULAR((2 * layers,)),
        ],
        compiler_params=pltpu.CompilerParams(collective_id=0, has_side_effects=True, vmem_limit_bytes=VMEM_LIMIT),
        name="layers",
    )(x, w_q, w_k, w_v, w_o, w_up, w_down, b_qkv, b_up, b_sum, gain, bias, *tables)


def rotary_tables(rows):
    half = rows // 2
    way, core, row = jnp.meshgrid(jnp.arange(2), jnp.arange(2), jnp.arange(half), indexing="ij")
    offset = (core * rows + way * half + row).astype(F32).reshape(2, rows, 1)
    base = (jnp.arange(RING, dtype=F32) * (2 * rows)).reshape(RING, 1, 1)
    lane = jnp.arange(LANES)
    pair = (lane % (ROT_DIM // 2)).astype(F32)
    inv_freq = jnp.where(lane < ROT_DIM, 1.0 / (ROPE_BASE ** (pair * (2.0 / ROT_DIM))), 0.0)
    return jnp.cos(base * inv_freq), jnp.sin(base * inv_freq), jnp.cos(offset * inv_freq), jnp.sin(offset * inv_freq)


def solution(mesh):
    head_spec = P(None, None, "tp", None)
    head_bias_spec = P(None, "tp", None)
    in_specs = (P("dp", "tp", None), P(), P(), head_spec, head_bias_spec, head_spec, head_bias_spec, head_spec, head_bias_spec,
                P(None, "tp", None, None), P(), P(None, None, "tp"), P(None, "tp"), P(None, "tp", None), P())

    def local_program(x_loc, ln_gain, ln_bias, w_q, b_q, w_k, b_k, w_v, b_v, w_o, b_o, w_up, b_up, w_down, b_down):
        layers, _, heads, head_dim = w_q.shape
        spare = LANES - head_dim

        def heads_first(weight):
            return jnp.transpose(weight, (0, 2, 3, 1))

        def wide_bias(vector, fill):
            lane = jnp.arange(LANES)
            padded = jnp.pad(vector.astype(F32), ((0, 0), (0, 0), (0, spare)))
            return jnp.where(lane == head_dim, fill, padded).reshape(layers, 1, heads * LANES)

        def row(vector):
            return vector.astype(F32).reshape(layers, 1, -1)

        b_qkv = jnp.concatenate([wide_bias(b_q, 0.0), wide_bias(b_k, 0.0), wide_bias(b_v, 1.0)], axis=2)
        out = run_layers(x_loc[0], heads_first(w_q), heads_first(w_k), heads_first(w_v), w_o, w_up, w_down, b_qkv, row(b_up),
                         row(b_o) + row(b_down), row(ln_gain), row(ln_bias), rotary_tables(x_loc.shape[1]))
        return out[None]

    return jax.shard_map(local_program, mesh=mesh, in_specs=in_specs, out_specs=P("dp", "tp", None), check_vma=False)
```

```python
import functools

import jax
import jax.numpy as jnp
from jax import lax
from jax.experimental import pallas as pl
from jax.experimental.pallas import tpu as pltpu
from jax.sharding import PartitionSpec as P

ROT_DIM = 32
ROPE_BASE = 10000.0
LN_EPS = 1e-5
LANES = 128
RING = 8
LOG2_E = 1.4426950408889634
MESH = pl.DeviceIdType.MESH
VMEM_LIMIT = 67043328
F32 = jnp.float32
BF16 = jnp.bfloat16


def ring_to_chip(pos):
    y = ((pos + 3) // 4) % 2
    z = y * (pos - 1) + (1 - y) * ((RING - pos) % RING)
    return 2 * z + y


def chip_to_ring(chip):
    y = chip % 2
    z = chip // 2
    return y * (z + 1) + (1 - y) * ((RING - z) % RING)


def place():
    me = lax.axis_index("tp")
    core = me % 2
    chip = me // 2
    pos = chip_to_ring(chip)
    right = 2 * ring_to_chip((pos + 1) % RING) + core
    left = 2 * ring_to_chip((pos + RING - 1) % RING) + core
    partner = 2 * chip + (1 - core)
    return core, chip, pos, right, left, partner


def meet(right, left, partner):
    barrier = pltpu.get_barrier_semaphore()
    for other in (right, left, partner):
        pl.semaphore_signal(barrier, inc=1, device_id={"tp": other}, device_id_type=MESH)
    pl.semaphore_wait(barrier, 3)


def layer_norm(hidden, gain, bias):
    x_f32 = hidden.astype(F32)
    mean = jnp.mean(x_f32, axis=-1, keepdims=True)
    centered = x_f32 - mean
    variance = jnp.mean(centered * centered, axis=-1, keepdims=True)
    return (centered * lax.rsqrt(variance + LN_EPS) * gain + bias).astype(BF16)


def layers_kernel(x_ref, wq_hbm, wk_hbm, wv_hbm, wo_hbm, wup_hbm, wdown_hbm, bq_ref, bk_ref, bv_ref, bup_ref, bo_ref, bdown_ref,
                  gain_ref, bias_ref, base_cos, base_sin, step_cos, step_sin, out_ref,
                  b_qkv, b_up, b_sum, gain, bias, hbuf, q_all, k_all, v_all, m_all, staged, w_qkv, w_up, w_o, w_down, given, own, acc, top,
                  weight_sem, gather_send, gather_recv, share_send, share_recv,
                  scatter_send, scatter_recv, pair_send, pair_recv, ready):
    layers, heads, head_dim, depth = wq_hbm.shape
    rows = x_ref.shape[0]
    half = rows // 2
    piece = half // 2
    width = heads * LANES
    tile = next(t for t in (512, 256, 128) if depth % t == 0)
    scale = head_dim ** -0.5 * LOG2_E
    core, chip, pos, right, left, partner = place()
    mine, other = pl.ds(pl.multiple_of(core * half, half), half), pl.ds(pl.multiple_of((1 - core) * half, half), half)

    def span_of(part):
        return pl.ds(pl.multiple_of(part * piece, piece), piece)

    def remote(src, dst, send_sem, recv_sem, to):
        return pltpu.make_async_remote_copy(src_ref=src, dst_ref=dst, send_sem=send_sem, recv_sem=recv_sem,
                                            device_id={"tp": to}, device_id_type=MESH)

    def next_of(way):
        return right if way == 0 else left

    def in_copies(layer):
        copies = [pltpu.make_async_copy(hbm.at[layer, head], staged.at[which * heads + head, pl.ds(0, head_dim)],
                                        weight_sem.at[which * heads + head])
                  for which, hbm in enumerate((wq_hbm, wk_hbm, wv_hbm)) for head in range(heads)]
        return copies + [pltpu.make_async_copy(wup_hbm.at[layer], w_up, weight_sem.at[3 * heads])]

    def out_copies(layer):
        copies = [pltpu.make_async_copy(wo_hbm.at[layer, head], w_o.at[pl.ds(head * LANES, head_dim)],
                                        weight_sem.at[3 * heads + 1 + head]) for head in range(heads)]
        return copies + [pltpu.make_async_copy(wdown_hbm.at[layer], w_down, weight_sem.at[4 * heads + 1])]

    def gathered_block(way, step):
        return ring_to_chip((pos + (1 - way) * (RING - step) + way * step) % RING)

    def gather_copy(way, step, sem_step, part):
        ref = hbuf.at[way, gathered_block(way, step), pl.ds(pl.multiple_of(core * half + part * piece, piece), piece)]
        return remote(ref, ref, gather_send.at[way, sem_step, part], gather_recv.at[way, sem_step, part], next_of(way))

    def share_copy(way, step, part, side):
        ref = hbuf.at[way, gathered_block(way, step), pl.ds(pl.multiple_of(side * half + part * piece, piece), piece)]
        return remote(ref, ref, share_send.at[way, step, part], share_recv.at[way, step, part], partner)

    def rotate(value, cosine, sine):
        lane = lax.broadcasted_iota(jnp.int32, value.shape, 1)
        swapped = jnp.where(lane < ROT_DIM // 2, pltpu.roll(value, LANES - ROT_DIM // 2, 1), pltpu.roll(value, ROT_DIM // 2, 1))
        return value * cosine + swapped * sine

    def project(layer, way, step):
        for part in range(2):
            share_copy(way, step, part, 1 - core).wait_recv()
        at = gathered_block(way, step)
        normed = hbuf[way, at]
        cos_0, sin_0, cos_1, sin_1 = base_cos[at], base_sin[at], step_cos[way], step_sin[way]
        lane = lax.broadcasted_iota(jnp.int32, (1, LANES), 1)
        sign = jnp.where(lane < ROT_DIM // 2, -1.0, 1.0)
        cosine = cos_0 * cos_1 - sin_0 * sin_1
        sine = (sin_0 * cos_1 + cos_0 * sin_1) * sign
        for which, out in enumerate((q_all, k_all, v_all)):
            cols = slice(which * width, (which + 1) * width)
            proj = jnp.dot(normed, w_qkv[:, cols], preferred_element_type=F32) + b_qkv[layer, :, cols]
            if which < 2:
                for head in range(heads):
                    lanes = slice(head * LANES, (head + 1) * LANES)
                    turned = rotate(proj[:, lanes], cosine, sine)
                    if which == 0:
                        out[at, way, lanes] = turned.T.astype(BF16)
                    else:
                        out[at, way, :, lanes] = turned.astype(BF16)
            else:
                for head in range(heads):
                    lanes = slice(head * LANES, (head + 1) * LANES)
                    out[at, way, lanes] = proj[:, lanes].T.astype(BF16)
        up = jnp.dot(normed, w_up[...], preferred_element_type=F32) + b_up[layer]
        m_all[at, way] = jax.nn.gelu(up, approximate=True).astype(BF16)

    def scattered_block(way, step):
        return ring_to_chip((pos + (1 - way) * (2 * RING - 1 - step) + way * (1 + step)) % RING)

    def scatter_copy(way, step, part):
        span = span_of(part)
        return remote(hbuf.at[way, step, span], hbuf.at[way, step + 1, span],
                      scatter_send.at[way, step, part], scatter_recv.at[way, step, part], next_of(way))

    def pair_copy(way, step):
        return remote(given.at[way, step % 2], hbuf.at[way, step, pl.ds(half, half)],
                      pair_send.at[way, step], pair_recv.at[way, step], partner)

    def fresh(way, slot):
        acc[way, slot] = jnp.zeros((heads, LANES, rows), F32)
        top[way, slot] = jnp.full((heads, 1, rows), -1e30, F32)

    def attend(way, slot, at, block, diagonal):
        if diagonal:
            key = lax.broadcasted_iota(jnp.int32, (2 * rows, 1), 0)
            key_pos = ((key // half) % 2) * (2 * half) + (key // rows) * half + key % half
            query = lax.broadcasted_iota(jnp.int32, (1, rows), 1)
            query_pos = ((query // half + core) % 2) * (2 * half) + way * half + query % half
            seen = query_pos >= key_pos
        for head in range(heads):
            lanes = slice(head * LANES, (head + 1) * LANES)
            queries = jnp.concatenate([q_all[at, way, lanes, mine], q_all[at, way, lanes, other]], axis=1)
            keys = k_all[block, :, :, lanes].reshape(2 * rows, LANES)
            score = jnp.dot(keys, queries, preferred_element_type=F32) * scale
            if diagonal:
                score = jnp.where(seen, score, -1e30)
            before = top[way, slot, head]
            peak = jnp.maximum(before, jnp.max(score, axis=0, keepdims=True))
            prob = jnp.exp2(score - peak).astype(BF16)
            weighed = (jnp.dot(v_all[block, 0, lanes], prob[:rows], preferred_element_type=F32)
                       + jnp.dot(v_all[block, 1, lanes], prob[rows:], preferred_element_type=F32))
            acc[way, slot, head] = acc[way, slot, head] * jnp.exp2(before - peak) + weighed
            top[way, slot, head] = peak

    def attend_ahead(offset):
        block = ring_to_chip((pos + offset) % RING)

        def queries_of(unit, carry):
            way, step = unit % 2, unit // 2
            at = scattered_block(way, step)

            @pl.when(block < at)
            def _():
                attend(way, step, at, block, False)

            return carry

        lax.fori_loop(0, 4, queries_of, 0)

    def attended_by(way, step):
        at, slot = scattered_block(way, step), step % 2

        @pl.when(step >= 2)
        def _():
            fresh(way, slot)

            def body(earlier, carry):
                attend(way, slot, at, earlier, False)
                return carry

            lax.fori_loop(0, at, body, 0)

        attend(way, slot, at, at, True)
        done = []
        for head in range(heads):
            sums = acc[way, slot, head]
            done.append((sums / sums[head_dim:head_dim + 1]).T.astype(BF16))
        return jnp.concatenate(done, axis=1)

    def contribute(way, step, before_send):
        at = scattered_block(way, step)
        attended = attended_by(way, step)
        up = jnp.concatenate([m_all[at, way, mine], m_all[at, way, other]], axis=0)

        @pl.when(step >= 2)
        def _():
            pair_copy(way, step - 2).wait_send()

        for low in range(0, depth, tile):
            cols = slice(low, low + tile)
            part_sum = (jnp.dot(attended, w_o[:, cols], preferred_element_type=F32)
                        + jnp.dot(up, w_down[:, cols], preferred_element_type=F32))
            own[way, step % 2, :, cols] = part_sum[:half]
            given[way, step % 2, :, cols] = part_sum[half:].astype(BF16)
        before_send()
        pair_copy(way, step).start()

    def total(way, step, part):
        span = span_of(part)
        taken = pl.ds(pl.multiple_of(half + part * piece, piece), piece)
        return own[way, step % 2, span] + hbuf[way, step, taken].astype(F32) + hbuf[way, step, span].astype(F32)

    def tell(phase):
        for to in (right, left, partner):
            pl.semaphore_signal(ready.at[phase], inc=1, device_id={"tp": to}, device_id_type=MESH)

    for copy in in_copies(0):
        copy.start()
    for g in range(3 * heads):
        staged[g, head_dim:] = jnp.zeros((LANES - head_dim, depth), BF16)
    for head in range(heads):
        w_o[head * LANES + head_dim:(head + 1) * LANES] = jnp.zeros((LANES - head_dim, depth), BF16)
    for wide, ref in ((b_up, bup_ref), (gain, gain_ref), (bias, bias_ref)):
        rows_f32 = ref[...].astype(F32)
        for layer in range(layers):
            wide[layer] = rows_f32[layer:layer + 1]
    rows_f32 = bo_ref[...].astype(F32) + bdown_ref[...].astype(F32)
    for layer in range(layers):
        b_sum[layer] = rows_f32[layer:layer + 1]
    column = lax.broadcasted_iota(jnp.int32, (1, 3 * width), 1)
    for layer in range(layers):
        b_qkv[layer] = jnp.where((column >= 2 * width) & (column % LANES == head_dim), 1.0, 0.0)
        for which, ref in enumerate((bq_ref, bk_ref, bv_ref)):
            heads_f32 = ref[layer].astype(F32)
            for head in range(heads):
                low = which * width + head * LANES
                b_qkv[layer, :, low:low + head_dim] = heads_f32[head:head + 1]
    out_ref[...] = x_ref[...]
    meet(right, left, partner)

    def layer_body(layer, carry):
        for copy in out_copies(layer):
            copy.start()
        for way in range(2):
            for part in range(2):
                low = way * half + part * piece
                hbuf[way, chip, pl.ds(pl.multiple_of(core * half + part * piece, piece), piece)] = layer_norm(
                    out_ref[low:low + piece], gain[layer], bias[layer])

        @pl.when(layer > 0)
        def _():
            pl.semaphore_wait(ready.at[2 * layer - 1], 3)

        for part in range(2):
            for way in range(2):
                gather_copy(way, 0, 0, part).start()
                share_copy(way, 0, part, core).start()

        for copy in in_copies(layer):
            copy.wait()
        for g in range(3 * heads):
            w_qkv[:, g * LANES:(g + 1) * LANES] = staged[g].T

        def arrive(event):
            step, part = 1 + event // 2, event % 2
            for way in range(2):
                gather_copy(way, step, step - 1, part).wait_recv()

                @pl.when(step < RING - 1)
                def _():
                    gather_copy(way, step, step, part).start()

                share_copy(way, step, part, core).start()

        def first_units(unit, carry):
            project(layer, unit, 0)
            return carry

        def events(event, carry):
            arrive(event)
            project(layer, (event + 1) % 2, (event + 1) // 2)

            @pl.when(event >= RING)
            def _():
                far, odd = (event - RING) // 2, event % 2
                attend_ahead((1 - odd) * (RING // 2 - far) + odd * (RING // 2 + far) * ((far + 1) // 2))

            return carry

        def nearest(side, carry):
            attend_ahead(1 + side * (RING - 2))
            return carry

        for way in range(2):
            for slot in range(2):
                fresh(way, slot)

        lax.fori_loop(0, 2, first_units, 0)
        arrive(0)
        lax.fori_loop(1, 2 * RING - 2, events, 0)
        project(layer, 1, RING - 1)
        lax.fori_loop(0, 2, nearest, 0)

        def drain_gather(step, carry):
            for way in range(2):
                for part in range(2):
                    @pl.when(step < RING - 1)
                    def _():
                        gather_copy(way, step, step, part).wait_send()

                    share_copy(way, step, part, core).wait_send()
            return carry

        lax.fori_loop(0, RING, drain_gather, 0)
        tell(2 * layer)

        @pl.when(layer < layers - 1)
        def _():
            for copy in in_copies(layer + 1):
                copy.start()

        for copy in out_copies(layer):
            copy.wait()
        for way in range(2):
            hbuf[way, 0, :half] = jnp.zeros((half, depth), BF16)

        def first_parts(way, carry):
            def before_send():
                @pl.when(way == 0)
                def _():
                    pl.semaphore_wait(ready.at[2 * layer], 3)

            contribute(way, 0, before_send)
            return carry

        def scatter_events(event, carry):
            step, part = event // 2, event % 2
            for way in range(2):
                @pl.when(part == 0)
                def _():
                    pair_copy(way, step).wait_recv()

                @pl.when(step > 0)
                def _():
                    scatter_copy(way, step - 1, part).wait_recv()

                hbuf[way, step, span_of(part)] = total(way, step, part).astype(BF16)
                scatter_copy(way, step, part).start()
            contribute(part, step + 1, lambda: None)
            return carry

        lax.fori_loop(0, 2, first_parts, 0)
        lax.fori_loop(0, 2 * RING - 2, scatter_events, 0)
        for part in range(2):
            for way in range(2):
                if part == 0:
                    pair_copy(way, RING - 1).wait_recv()
                scatter_copy(way, RING - 2, part).wait_recv()
                low = way * half + part * piece
                hidden = out_ref[low:low + piece].astype(F32) + total(way, RING - 1, part) + b_sum[layer]
                out_ref[low:low + piece] = hidden.astype(BF16)

        def drain_scatter(step, carry):
            for way in range(2):
                for part in range(2):
                    scatter_copy(way, step, part).wait_send()
            return carry

        lax.fori_loop(0, RING - 1, drain_scatter, 0)
        for way in range(2):
            for step in (RING - 2, RING - 1):
                pair_copy(way, step).wait_send()

        @pl.when(layer < layers - 1)
        def _():
            tell(2 * layer + 1)

        return carry

    lax.fori_loop(0, layers, layer_body, 0)


def run_layers(x, w_q, w_k, w_v, w_o, w_up, w_down, vectors, tables):
    rows, depth = x.shape
    layers, heads, head_dim, _ = w_q.shape
    width, hidden_width = heads * LANES, w_up.shape[2]
    half = rows // 2
    vmem = pl.BlockSpec(memory_space=pltpu.VMEM)
    hbm = pl.BlockSpec(memory_space=pl.ANY)
    return pl.pallas_call(
        layers_kernel,
        out_shape=jax.ShapeDtypeStruct((rows, depth), BF16),
        in_specs=[vmem] + [hbm] * 6 + [vmem] * 12,
        out_specs=vmem,
        scratch_shapes=[
            pltpu.VMEM((layers, 1, 3 * width), F32),
            pltpu.VMEM((layers, 1, hidden_width), F32),
            pltpu.VMEM((layers, 1, depth), F32),
            pltpu.VMEM((layers, 1, depth), F32),
            pltpu.VMEM((layers, 1, depth), F32),
            pltpu.VMEM((2, RING, rows, depth), BF16),
            pltpu.VMEM((RING, 2, width, rows), BF16),
            pltpu.VMEM((RING, 2, rows, width), BF16),
            pltpu.VMEM((RING, 2, width, rows), BF16),
            pltpu.VMEM((RING, 2, rows, hidden_width), BF16),
            pltpu.VMEM((3 * heads, LANES, depth), BF16),
            pltpu.VMEM((depth, 3 * width), BF16),
            pltpu.VMEM((depth, hidden_width), BF16),
            pltpu.VMEM((width, depth), BF16),
            pltpu.VMEM((hidden_width, depth), BF16),
            pltpu.VMEM((2, 2, half, depth), BF16),
            pltpu.VMEM((2, 2, half, depth), F32),
            pltpu.VMEM((2, 2, heads, LANES, rows), F32),
            pltpu.VMEM((2, 2, heads, 1, rows), F32),
            pltpu.SemaphoreType.DMA((4 * heads + 2,)),
            pltpu.SemaphoreType.DMA((2, RING, 2)),
            pltpu.SemaphoreType.DMA((2, RING, 2)),
            pltpu.SemaphoreType.DMA((2, RING, 2)),
            pltpu.SemaphoreType.DMA((2, RING, 2)),
            pltpu.SemaphoreType.DMA((2, RING, 2)),
            pltpu.SemaphoreType.DMA((2, RING, 2)),
            pltpu.SemaphoreType.DMA((2, RING)),
            pltpu.SemaphoreType.DMA((2, RING)),
            pltpu.SemaphoreType.REGULAR((2 * layers,)),
        ],
        compiler_params=pltpu.CompilerParams(collective_id=0, has_side_effects=True, vmem_limit_bytes=VMEM_LIMIT),
        name="layers",
    )(x, w_q, w_k, w_v, w_o, w_up, w_down, *vectors, *tables)


def rotary_tables(rows):
    half = rows // 2
    way, core, row = jnp.meshgrid(jnp.arange(2), jnp.arange(2), jnp.arange(half), indexing="ij")
    offset = (core * rows + way * half + row).astype(F32).reshape(2, rows, 1)
    base = (jnp.arange(RING, dtype=F32) * (2 * rows)).reshape(RING, 1, 1)
    lane = jnp.arange(LANES)
    pair = (lane % (ROT_DIM // 2)).astype(F32)
    inv_freq = jnp.where(lane < ROT_DIM, 1.0 / (ROPE_BASE ** (pair * (2.0 / ROT_DIM))), 0.0)
    return jnp.cos(base * inv_freq), jnp.sin(base * inv_freq), jnp.cos(offset * inv_freq), jnp.sin(offset * inv_freq)


def solution(mesh):
    head_spec = P(None, None, "tp", None)
    head_bias_spec = P(None, "tp", None)
    in_specs = (P("dp", "tp", None), P(), P(), head_spec, head_bias_spec, head_spec, head_bias_spec, head_spec, head_bias_spec,
                P(None, "tp", None, None), P(), P(None, None, "tp"), P(None, "tp"), P(None, "tp", None), P())

    def local_program(x_loc, ln_gain, ln_bias, w_q, b_q, w_k, b_k, w_v, b_v, w_o, b_o, w_up, b_up, w_down, b_down):
        def heads_first(weight):
            return jnp.transpose(weight, (0, 2, 3, 1))

        out = run_layers(x_loc[0], heads_first(w_q), heads_first(w_k), heads_first(w_v), w_o, w_up, w_down,
                         (b_q, b_k, b_v, b_up, b_o, b_down, ln_gain, ln_bias), rotary_tables(x_loc.shape[1]))
        return out[None]

    return jax.shard_map(local_program, mesh=mesh, in_specs=in_specs, out_specs=P("dp", "tp", None), check_vma=False)
```

```python
import functools

import jax
import jax.numpy as jnp
from jax import lax
from jax.experimental import pallas as pl
from jax.experimental.pallas import tpu as pltpu
from jax.sharding import PartitionSpec as P

ROT_DIM = 32
ROPE_BASE = 10000.0
LN_EPS = 1e-5
LANES = 128
RING = 8
PARTS = 4
LOG2_E = 1.4426950408889634
MESH = pl.DeviceIdType.MESH
VMEM_LIMIT = 67043328
F32 = jnp.float32
BF16 = jnp.bfloat16


def ring_to_chip(pos):
    y = ((pos + 3) // 4) % 2
    z = y * (pos - 1) + (1 - y) * ((RING - pos) % RING)
    return 2 * z + y


def chip_to_ring(chip):
    y = chip % 2
    z = chip // 2
    return y * (z + 1) + (1 - y) * ((RING - z) % RING)


def place():
    me = lax.axis_index("tp")
    core = me % 2
    chip = me // 2
    pos = chip_to_ring(chip)
    right = 2 * ring_to_chip((pos + 1) % RING) + core
    left = 2 * ring_to_chip((pos + RING - 1) % RING) + core
    partner = 2 * chip + (1 - core)
    return core, chip, pos, right, left, partner


def meet(right, left, partner):
    barrier = pltpu.get_barrier_semaphore()
    for other in (right, left, partner):
        pl.semaphore_signal(barrier, inc=1, device_id={"tp": other}, device_id_type=MESH)
    pl.semaphore_wait(barrier, 3)


def layer_norm(hidden, gain, bias):
    x_f32 = hidden.astype(F32)
    mean = jnp.mean(x_f32, axis=-1, keepdims=True)
    centered = x_f32 - mean
    variance = jnp.mean(centered * centered, axis=-1, keepdims=True)
    return (centered * lax.rsqrt(variance + LN_EPS) * gain + bias).astype(BF16)


def layers_kernel(x_ref, wq_hbm, wk_hbm, wv_hbm, wo_hbm, wup_hbm, wdown_hbm, bq_ref, bk_ref, bv_ref, bup_ref, bo_ref, bdown_ref,
                  gain_ref, bias_ref, base_cos, base_sin, step_cos, step_sin, out_ref,
                  b_qkv, b_up, b_sum, gain, bias, hbuf, q_all, k_all, v_all, m_all, staged, w_qkv, w_up, w_o, w_down, given, own, acc, top,
                  weight_sem, gather_send, gather_recv, share_send, share_recv,
                  scatter_send, scatter_recv, pair_send, pair_recv, ready):
    layers, heads, head_dim, depth = wq_hbm.shape
    rows = x_ref.shape[0]
    half = rows // 2
    piece = half // PARTS
    group = PARTS // 2
    width = heads * LANES
    tile = next(t for t in (512, 256, 128) if depth % t == 0)
    scale = head_dim ** -0.5 * LOG2_E
    core, chip, pos, right, left, partner = place()
    mine, other = pl.ds(pl.multiple_of(core * half, half), half), pl.ds(pl.multiple_of((1 - core) * half, half), half)

    def span_of(part):
        return pl.ds(pl.multiple_of(part * piece, piece), piece)

    def remote(src, dst, send_sem, recv_sem, to):
        return pltpu.make_async_remote_copy(src_ref=src, dst_ref=dst, send_sem=send_sem, recv_sem=recv_sem,
                                            device_id={"tp": to}, device_id_type=MESH)

    def next_of(way):
        return right if way == 0 else left

    def in_copies(layer):
        copies = [pltpu.make_async_copy(hbm.at[layer, head], staged.at[which * heads + head, pl.ds(0, head_dim)],
                                        weight_sem.at[which * heads + head])
                  for which, hbm in enumerate((wq_hbm, wk_hbm, wv_hbm)) for head in range(heads)]
        return copies + [pltpu.make_async_copy(wup_hbm.at[layer], w_up, weight_sem.at[3 * heads])]

    def out_copies(layer):
        copies = [pltpu.make_async_copy(wo_hbm.at[layer, head], w_o.at[pl.ds(head * LANES, head_dim)],
                                        weight_sem.at[3 * heads + 1 + head]) for head in range(heads)]
        return copies + [pltpu.make_async_copy(wdown_hbm.at[layer], w_down, weight_sem.at[4 * heads + 1])]

    def gathered_block(way, step):
        return ring_to_chip((pos + (1 - way) * (RING - step) + way * step) % RING)

    def gather_copy(way, step, sem_step, part):
        ref = hbuf.at[way, gathered_block(way, step), pl.ds(pl.multiple_of(core * half + part * piece, piece), piece)]
        return remote(ref, ref, gather_send.at[way, sem_step, part], gather_recv.at[way, sem_step, part], next_of(way))

    def share_copy(way, step, part, side):
        ref = hbuf.at[way, gathered_block(way, step), pl.ds(pl.multiple_of(side * half + part * piece, piece), piece)]
        return remote(ref, ref, share_send.at[way, step, part], share_recv.at[way, step, part], partner)

    def rotate(value, cosine, sine):
        lane = lax.broadcasted_iota(jnp.int32, value.shape, 1)
        swapped = jnp.where(lane < ROT_DIM // 2, pltpu.roll(value, LANES - ROT_DIM // 2, 1), pltpu.roll(value, ROT_DIM // 2, 1))
        return value * cosine + swapped * sine

    def project(layer, way, step):
        for part in range(PARTS):
            share_copy(way, step, part, 1 - core).wait_recv()
        at = gathered_block(way, step)
        normed = hbuf[way, at]
        cos_0, sin_0, cos_1, sin_1 = base_cos[at], base_sin[at], step_cos[way], step_sin[way]
        lane = lax.broadcasted_iota(jnp.int32, (1, LANES), 1)
        sign = jnp.where(lane < ROT_DIM // 2, -1.0, 1.0)
        cosine = cos_0 * cos_1 - sin_0 * sin_1
        sine = (sin_0 * cos_1 + cos_0 * sin_1) * sign
        for which, out in enumerate((q_all, k_all, v_all)):
            cols = slice(which * width, (which + 1) * width)
            proj = jnp.dot(normed, w_qkv[:, cols], preferred_element_type=F32) + b_qkv[layer, :, cols]
            if which < 2:
                for head in range(heads):
                    lanes = slice(head * LANES, (head + 1) * LANES)
                    turned = rotate(proj[:, lanes], cosine, sine)
                    if which == 0:
                        out[at, way, lanes] = turned.T.astype(BF16)
                    else:
                        out[at, way, :, lanes] = turned.astype(BF16)
            else:
                for head in range(heads):
                    lanes = slice(head * LANES, (head + 1) * LANES)
                    out[at, way, lanes] = proj[:, lanes].T.astype(BF16)
        up = jnp.dot(normed, w_up[...], preferred_element_type=F32) + b_up[layer]
        m_all[at, way] = jax.nn.gelu(up, approximate=True).astype(BF16)

    def scattered_block(way, step):
        return ring_to_chip((pos + (1 - way) * (2 * RING - 1 - step) + way * (1 + step)) % RING)

    def scatter_copy(way, step, part):
        span = span_of(part)
        return remote(hbuf.at[way, step, span], hbuf.at[way, step + 1, span],
                      scatter_send.at[way, step, part], scatter_recv.at[way, step, part], next_of(way))

    def pair_copy(way, step):
        return remote(given.at[way, step % 2], hbuf.at[way, step, pl.ds(half, half)],
                      pair_send.at[way, step], pair_recv.at[way, step], partner)

    def fresh(way, slot):
        acc[way, slot] = jnp.zeros((heads, LANES, rows), F32)
        top[way, slot] = jnp.full((heads, 1, rows), -1e30, F32)

    def attend(way, slot, at, block, diagonal):
        if diagonal:
            key = lax.broadcasted_iota(jnp.int32, (2 * rows, 1), 0)
            key_pos = ((key // half) % 2) * (2 * half) + (key // rows) * half + key % half
            query = lax.broadcasted_iota(jnp.int32, (1, rows), 1)
            query_pos = ((query // half + core) % 2) * (2 * half) + way * half + query % half
            seen = query_pos >= key_pos
        for head in range(heads):
            lanes = slice(head * LANES, (head + 1) * LANES)
            queries = jnp.concatenate([q_all[at, way, lanes, mine], q_all[at, way, lanes, other]], axis=1)
            keys = k_all[block, :, :, lanes].reshape(2 * rows, LANES)
            score = jnp.dot(keys, queries, preferred_element_type=F32) * scale
            if diagonal:
                score = jnp.where(seen, score, -1e30)
            before = top[way, slot, head]
            peak = jnp.maximum(before, jnp.max(score, axis=0, keepdims=True))
            prob = jnp.exp2(score - peak).astype(BF16)
            weighed = (jnp.dot(v_all[block, 0, lanes], prob[:rows], preferred_element_type=F32)
                       + jnp.dot(v_all[block, 1, lanes], prob[rows:], preferred_element_type=F32))
            acc[way, slot, head] = acc[way, slot, head] * jnp.exp2(before - peak) + weighed
            top[way, slot, head] = peak

    def attend_ahead(offset):
        block = ring_to_chip((pos + offset) % RING)

        def queries_of(unit, carry):
            way, step = unit % 2, unit // 2
            at = scattered_block(way, step)

            @pl.when(block < at)
            def _():
                attend(way, step, at, block, False)

            return carry

        lax.fori_loop(0, 4, queries_of, 0)

    def attended_by(way, step):
        at, slot = scattered_block(way, step), step % 2

        @pl.when(step >= 2)
        def _():
            fresh(way, slot)

            def body(earlier, carry):
                attend(way, slot, at, earlier, False)
                return carry

            lax.fori_loop(0, at, body, 0)

        attend(way, slot, at, at, True)
        done = []
        for head in range(heads):
            sums = acc[way, slot, head]
            done.append((sums / sums[head_dim:head_dim + 1]).T.astype(BF16))
        return jnp.concatenate(done, axis=1)

    def contribute(way, step, before_send):
        at = scattered_block(way, step)
        attended = attended_by(way, step)
        up = jnp.concatenate([m_all[at, way, mine], m_all[at, way, other]], axis=0)

        @pl.when(step >= 2)
        def _():
            pair_copy(way, step - 2).wait_send()

        for low in range(0, depth, tile):
            cols = slice(low, low + tile)
            part_sum = (jnp.dot(attended, w_o[:, cols], preferred_element_type=F32)
                        + jnp.dot(up, w_down[:, cols], preferred_element_type=F32))
            own[way, step % 2, :, cols] = part_sum[:half]
            given[way, step % 2, :, cols] = part_sum[half:].astype(BF16)
        before_send()
        pair_copy(way, step).start()

    def total(way, step, part):
        span = span_of(part)
        taken = pl.ds(pl.multiple_of(half + part * piece, piece), piece)
        return own[way, step % 2, span] + hbuf[way, step, taken].astype(F32) + hbuf[way, step, span].astype(F32)

    def tell(phase):
        for to in (right, left, partner):
            pl.semaphore_signal(ready.at[phase], inc=1, device_id={"tp": to}, device_id_type=MESH)

    for copy in in_copies(0):
        copy.start()
    for g in range(3 * heads):
        staged[g, head_dim:] = jnp.zeros((LANES - head_dim, depth), BF16)
    for head in range(heads):
        w_o[head * LANES + head_dim:(head + 1) * LANES] = jnp.zeros((LANES - head_dim, depth), BF16)
    for wide, ref in ((b_up, bup_ref), (gain, gain_ref), (bias, bias_ref)):
        rows_f32 = ref[...].astype(F32)
        for layer in range(layers):
            wide[layer] = rows_f32[layer:layer + 1]
    rows_f32 = bo_ref[...].astype(F32) + bdown_ref[...].astype(F32)
    for layer in range(layers):
        b_sum[layer] = rows_f32[layer:layer + 1]
    column = lax.broadcasted_iota(jnp.int32, (1, 3 * width), 1)
    for layer in range(layers):
        b_qkv[layer] = jnp.where((column >= 2 * width) & (column % LANES == head_dim), 1.0, 0.0)
        for which, ref in enumerate((bq_ref, bk_ref, bv_ref)):
            heads_f32 = ref[layer].astype(F32)
            for head in range(heads):
                low = which * width + head * LANES
                b_qkv[layer, :, low:low + head_dim] = heads_f32[head:head + 1]
    out_ref[...] = x_ref[...]
    meet(right, left, partner)

    def layer_body(layer, carry):
        for copy in out_copies(layer):
            copy.start()
        for way in range(2):
            for part in range(PARTS):
                low = way * half + part * piece
                hbuf[way, chip, pl.ds(pl.multiple_of(core * half + part * piece, piece), piece)] = layer_norm(
                    out_ref[low:low + piece], gain[layer], bias[layer])

        @pl.when(layer > 0)
        def _():
            pl.semaphore_wait(ready.at[2 * layer - 1], 3)

        for part in range(PARTS):
            for way in range(2):
                gather_copy(way, 0, 0, part).start()
                share_copy(way, 0, part, core).start()

        for copy in in_copies(layer):
            copy.wait()
        for g in range(3 * heads):
            w_qkv[:, g * LANES:(g + 1) * LANES] = staged[g].T

        def arrive(event):
            step = 1 + event // 2
            for index in range(group):
                part = event % 2 * group + index
                for way in range(2):
                    gather_copy(way, step, step - 1, part).wait_recv()

                    @pl.when(step < RING - 1)
                    def _():
                        gather_copy(way, step, step, part).start()

                    share_copy(way, step, part, core).start()

        def first_units(unit, carry):
            project(layer, unit, 0)
            return carry

        def events(event, carry):
            arrive(event)
            project(layer, (event + 1) % 2, (event + 1) // 2)

            @pl.when(event >= RING)
            def _():
                far, odd = (event - RING) // 2, event % 2
                attend_ahead((1 - odd) * (RING // 2 - far) + odd * (RING // 2 + far) * ((far + 1) // 2))

            return carry

        def nearest(side, carry):
            attend_ahead(1 + side * (RING - 2))
            return carry

        for way in range(2):
            for slot in range(2):
                fresh(way, slot)

        lax.fori_loop(0, 2, first_units, 0)
        arrive(0)
        lax.fori_loop(1, 2 * RING - 2, events, 0)
        project(layer, 1, RING - 1)
        lax.fori_loop(0, 2, nearest, 0)

        def drain_gather(step, carry):
            for way in range(2):
                for part in range(PARTS):
                    @pl.when(step < RING - 1)
                    def _():
                        gather_copy(way, step, step, part).wait_send()

                    share_copy(way, step, part, core).wait_send()
            return carry

        lax.fori_loop(0, RING, drain_gather, 0)
        tell(2 * layer)

        @pl.when(layer < layers - 1)
        def _():
            for copy in in_copies(layer + 1):
                copy.start()

        for copy in out_copies(layer):
            copy.wait()
        for way in range(2):
            hbuf[way, 0, :half] = jnp.zeros((half, depth), BF16)

        def first_parts(way, carry):
            def before_send():
                @pl.when(way == 0)
                def _():
                    pl.semaphore_wait(ready.at[2 * layer], 3)

            contribute(way, 0, before_send)
            return carry

        def scatter_events(event, carry):
            step, second = event // 2, event % 2
            for index in range(group):
                part = second * group + index
                for way in range(2):
                    if index == 0:
                        @pl.when(second == 0)
                        def _():
                            pair_copy(way, step).wait_recv()

                    @pl.when(step > 0)
                    def _():
                        scatter_copy(way, step - 1, part).wait_recv()

                    hbuf[way, step, span_of(part)] = total(way, step, part).astype(BF16)
                    scatter_copy(way, step, part).start()
            contribute(second, step + 1, lambda: None)
            return carry

        lax.fori_loop(0, 2, first_parts, 0)
        lax.fori_loop(0, 2 * RING - 2, scatter_events, 0)
        for part in range(PARTS):
            for way in range(2):
                if part == 0:
                    pair_copy(way, RING - 1).wait_recv()
                scatter_copy(way, RING - 2, part).wait_recv()
                low = way * half + part * piece
                hidden = out_ref[low:low + piece].astype(F32) + total(way, RING - 1, part) + b_sum[layer]
                out_ref[low:low + piece] = hidden.astype(BF16)

        def drain_scatter(step, carry):
            for way in range(2):
                for part in range(PARTS):
                    scatter_copy(way, step, part).wait_send()
            return carry

        lax.fori_loop(0, RING - 1, drain_scatter, 0)
        for way in range(2):
            for step in (RING - 2, RING - 1):
                pair_copy(way, step).wait_send()

        @pl.when(layer < layers - 1)
        def _():
            tell(2 * layer + 1)

        return carry

    lax.fori_loop(0, layers, layer_body, 0)


def run_layers(x, w_q, w_k, w_v, w_o, w_up, w_down, vectors, tables):
    rows, depth = x.shape
    layers, heads, head_dim, _ = w_q.shape
    width, hidden_width = heads * LANES, w_up.shape[2]
    half = rows // 2
    vmem = pl.BlockSpec(memory_space=pltpu.VMEM)
    hbm = pl.BlockSpec(memory_space=pl.ANY)
    return pl.pallas_call(
        layers_kernel,
        out_shape=jax.ShapeDtypeStruct((rows, depth), BF16),
        in_specs=[vmem] + [hbm] * 6 + [vmem] * 12,
        out_specs=vmem,
        scratch_shapes=[
            pltpu.VMEM((layers, 1, 3 * width), F32),
            pltpu.VMEM((layers, 1, hidden_width), F32),
            pltpu.VMEM((layers, 1, depth), F32),
            pltpu.VMEM((layers, 1, depth), F32),
            pltpu.VMEM((layers, 1, depth), F32),
            pltpu.VMEM((2, RING, rows, depth), BF16),
            pltpu.VMEM((RING, 2, width, rows), BF16),
            pltpu.VMEM((RING, 2, rows, width), BF16),
            pltpu.VMEM((RING, 2, width, rows), BF16),
            pltpu.VMEM((RING, 2, rows, hidden_width), BF16),
            pltpu.VMEM((3 * heads, LANES, depth), BF16),
            pltpu.VMEM((depth, 3 * width), BF16),
            pltpu.VMEM((depth, hidden_width), BF16),
            pltpu.VMEM((width, depth), BF16),
            pltpu.VMEM((hidden_width, depth), BF16),
            pltpu.VMEM((2, 2, half, depth), BF16),
            pltpu.VMEM((2, 2, half, depth), F32),
            pltpu.VMEM((2, 2, heads, LANES, rows), F32),
            pltpu.VMEM((2, 2, heads, 1, rows), F32),
            pltpu.SemaphoreType.DMA((4 * heads + 2,)),
            pltpu.SemaphoreType.DMA((2, RING, PARTS)),
            pltpu.SemaphoreType.DMA((2, RING, PARTS)),
            pltpu.SemaphoreType.DMA((2, RING, PARTS)),
            pltpu.SemaphoreType.DMA((2, RING, PARTS)),
            pltpu.SemaphoreType.DMA((2, RING, PARTS)),
            pltpu.SemaphoreType.DMA((2, RING, PARTS)),
            pltpu.SemaphoreType.DMA((2, RING)),
            pltpu.SemaphoreType.DMA((2, RING)),
            pltpu.SemaphoreType.REGULAR((2 * layers,)),
        ],
        compiler_params=pltpu.CompilerParams(collective_id=0, has_side_effects=True, vmem_limit_bytes=VMEM_LIMIT),
        name="layers",
    )(x, w_q, w_k, w_v, w_o, w_up, w_down, *vectors, *tables)


def rotary_tables(rows):
    half = rows // 2
    way, core, row = jnp.meshgrid(jnp.arange(2), jnp.arange(2), jnp.arange(half), indexing="ij")
    offset = (core * rows + way * half + row).astype(F32).reshape(2, rows, 1)
    base = (jnp.arange(RING, dtype=F32) * (2 * rows)).reshape(RING, 1, 1)
    lane = jnp.arange(LANES)
    pair = (lane % (ROT_DIM // 2)).astype(F32)
    inv_freq = jnp.where(lane < ROT_DIM, 1.0 / (ROPE_BASE ** (pair * (2.0 / ROT_DIM))), 0.0)
    return jnp.cos(base * inv_freq), jnp.sin(base * inv_freq), jnp.cos(offset * inv_freq), jnp.sin(offset * inv_freq)


def solution(mesh):
    head_spec = P(None, None, "tp", None)
    head_bias_spec = P(None, "tp", None)
    in_specs = (P("dp", "tp", None), P(), P(), head_spec, head_bias_spec, head_spec, head_bias_spec, head_spec, head_bias_spec,
                P(None, "tp", None, None), P(), P(None, None, "tp"), P(None, "tp"), P(None, "tp", None), P())

    def local_program(x_loc, ln_gain, ln_bias, w_q, b_q, w_k, b_k, w_v, b_v, w_o, b_o, w_up, b_up, w_down, b_down):
        def heads_first(weight):
            return jnp.transpose(weight, (0, 2, 3, 1))

        out = run_layers(x_loc[0], heads_first(w_q), heads_first(w_k), heads_first(w_v), w_o, w_up, w_down,
                         (b_q, b_k, b_v, b_up, b_o, b_down, ln_gain, ln_bias), rotary_tables(x_loc.shape[1]))
        return out[None]

    return jax.shard_map(local_program, mesh=mesh, in_specs=in_specs, out_specs=P("dp", "tp", None), check_vma=False)
```

```python
import functools

import jax
import jax.numpy as jnp
from jax import lax
from jax.experimental import pallas as pl
from jax.experimental.pallas import tpu as pltpu
from jax.sharding import PartitionSpec as P

ROT_DIM = 32
ROPE_BASE = 10000.0
LN_EPS = 1e-5
LANES = 128
RING = 8
PARTS = 2
LOG2_E = 1.4426950408889634
MESH = pl.DeviceIdType.MESH
VMEM_LIMIT = 67043328
F32 = jnp.float32
BF16 = jnp.bfloat16


def ring_to_chip(pos):
    y = ((pos + 3) // 4) % 2
    z = y * (pos - 1) + (1 - y) * ((RING - pos) % RING)
    return 2 * z + y


def chip_to_ring(chip):
    y = chip % 2
    z = chip // 2
    return y * (z + 1) + (1 - y) * ((RING - z) % RING)


def place():
    me = lax.axis_index("tp")
    core = me % 2
    chip = me // 2
    pos = chip_to_ring(chip)
    right = 2 * ring_to_chip((pos + 1) % RING) + core
    left = 2 * ring_to_chip((pos + RING - 1) % RING) + core
    partner = 2 * chip + (1 - core)
    return core, chip, pos, right, left, partner


def call(right, left, partner):
    barrier = pltpu.get_barrier_semaphore()
    for other in (right, left, partner):
        pl.semaphore_signal(barrier, inc=1, device_id={"tp": other}, device_id_type=MESH)
    return barrier


def layer_norm(hidden, gain, bias):
    x_f32 = hidden.astype(F32)
    mean = jnp.mean(x_f32, axis=-1, keepdims=True)
    centered = x_f32 - mean
    variance = jnp.mean(centered * centered, axis=-1, keepdims=True)
    return (centered * lax.rsqrt(variance + LN_EPS) * gain + bias).astype(BF16)


def layers_kernel(x_ref, wq_hbm, wk_hbm, wv_hbm, wo_hbm, wup_hbm, wdown_hbm, bq_ref, bk_ref, bv_ref, bup_ref, bo_ref, bdown_ref,
                  gain_ref, bias_ref, base_cos, base_sin, step_cos, step_sin, out_ref,
                  b_qkv, b_up, b_sum, gain, bias, hbuf, q_all, k_all, v_all, m_all, staged, w_qkv, w_up, w_o, w_down, given, own, acc, top,
                  weight_sem, gather_send, gather_recv, share_send, share_recv,
                  scatter_send, scatter_recv, pair_send, pair_recv, ready):
    layers, heads, head_dim, depth = wq_hbm.shape
    rows = x_ref.shape[0]
    half = rows // 2
    piece = half // PARTS
    group = PARTS // 2
    width = heads * LANES
    tile = next(t for t in (512, 256, 128) if depth % t == 0)
    scale = head_dim ** -0.5 * LOG2_E
    core, chip, pos, right, left, partner = place()
    mine, other = pl.ds(pl.multiple_of(core * half, half), half), pl.ds(pl.multiple_of((1 - core) * half, half), half)

    def span_of(part):
        return pl.ds(pl.multiple_of(part * piece, piece), piece)

    def remote(src, dst, send_sem, recv_sem, to):
        return pltpu.make_async_remote_copy(src_ref=src, dst_ref=dst, send_sem=send_sem, recv_sem=recv_sem,
                                            device_id={"tp": to}, device_id_type=MESH)

    def next_of(way):
        return right if way == 0 else left

    def in_copies(layer):
        copies = [pltpu.make_async_copy(hbm.at[layer, head], staged.at[which * heads + head, pl.ds(0, head_dim)],
                                        weight_sem.at[which * heads + head])
                  for which, hbm in enumerate((wq_hbm, wk_hbm, wv_hbm)) for head in range(heads)]
        return copies + [pltpu.make_async_copy(wup_hbm.at[layer], w_up, weight_sem.at[3 * heads])]

    def out_copies(layer):
        copies = [pltpu.make_async_copy(wo_hbm.at[layer, head], w_o.at[pl.ds(head * LANES, head_dim)],
                                        weight_sem.at[3 * heads + 1 + head]) for head in range(heads)]
        return copies + [pltpu.make_async_copy(wdown_hbm.at[layer], w_down, weight_sem.at[4 * heads + 1])]

    def gathered_block(way, step):
        return ring_to_chip((pos + (1 - way) * (RING - step) + way * step) % RING)

    def gather_rows(way, step, part, side):
        return hbuf.at[way, step, pl.ds(pl.multiple_of(side * half + part * piece, piece), piece)]

    def gather_copy(way, step, part):
        return remote(gather_rows(way, step, part, core), gather_rows(way, step + 1, part, core),
                      gather_send.at[way, step, part], gather_recv.at[way, step, part], next_of(way))

    def share_copy(way, step, part, side):
        ref = gather_rows(way, step, part, side)
        return remote(ref, ref, share_send.at[way, step, part], share_recv.at[way, step, part], partner)

    def rotate(value, cosine, sine):
        lane = lax.broadcasted_iota(jnp.int32, value.shape, 1)
        swapped = jnp.where(lane < ROT_DIM // 2, pltpu.roll(value, LANES - ROT_DIM // 2, 1), pltpu.roll(value, ROT_DIM // 2, 1))
        return value * cosine + swapped * sine

    def turning(way, at):
        cos_0, sin_0, cos_1, sin_1 = base_cos[at], base_sin[at], step_cos[way], step_sin[way]
        lane = lax.broadcasted_iota(jnp.int32, (1, LANES), 1)
        sign = jnp.where(lane < ROT_DIM // 2, -1.0, 1.0)
        return cos_0 * cos_1 - sin_0 * sin_1, (sin_0 * cos_1 + cos_0 * sin_1) * sign

    def project(layer, way, step, which):
        cols = slice(which * width, (which + 1) * width)
        return jnp.dot(hbuf[way, step], w_qkv[:, cols], preferred_element_type=F32) + b_qkv[layer, :, cols]

    def project_kv(layer, way, step):
        for part in range(PARTS):
            share_copy(way, step, part, 1 - core).wait_recv()
        at = gathered_block(way, step)
        cosine, sine = turning(way, at)
        keys, values = project(layer, way, step, 1), project(layer, way, step, 2)
        for head in range(heads):
            lanes = slice(head * LANES, (head + 1) * LANES)
            k_all[at, way, :, lanes] = rotate(keys[:, lanes], cosine, sine).astype(BF16)
            v_all[at, way, lanes] = values[:, lanes].T.astype(BF16)

    def project_rest(layer, way, step):
        at = gathered_block(way, step)
        cosine, sine = turning(way, at)
        queries = project(layer, way, step, 0)
        for head in range(heads):
            lanes = slice(head * LANES, (head + 1) * LANES)
            q_all[at, way, lanes] = rotate(queries[:, lanes], cosine, sine).T.astype(BF16)
        up = jnp.dot(hbuf[way, step], w_up[...], preferred_element_type=F32) + b_up[layer]
        m_all[at, way] = jax.nn.gelu(up, approximate=True).astype(BF16)

    def scattered_block(way, step):
        return ring_to_chip((pos + (1 - way) * (2 * RING - 1 - step) + way * (1 + step)) % RING)

    def scatter_copy(way, step, part):
        span = span_of(part)
        return remote(hbuf.at[way, step, span], hbuf.at[way, step + 1, span],
                      scatter_send.at[way, step, part], scatter_recv.at[way, step, part], next_of(way))

    def pair_copy(way, step):
        return remote(given.at[way, step % 2], hbuf.at[way, step, pl.ds(half, half)],
                      pair_send.at[way, step], pair_recv.at[way, step], partner)

    def fresh(way, slot):
        acc[way, slot] = jnp.zeros((heads, LANES, rows), F32)
        top[way, slot] = jnp.full((heads, 1, rows), -1e30, F32)

    def attend(way, slot, at, block, diagonal):
        if diagonal:
            key = lax.broadcasted_iota(jnp.int32, (2 * rows, 1), 0)
            key_pos = ((key // half) % 2) * (2 * half) + (key // rows) * half + key % half
            query = lax.broadcasted_iota(jnp.int32, (1, rows), 1)
            query_pos = ((query // half + core) % 2) * (2 * half) + way * half + query % half
            seen = query_pos >= key_pos
        for head in range(heads):
            lanes = slice(head * LANES, (head + 1) * LANES)
            queries = jnp.concatenate([q_all[at, way, lanes, mine], q_all[at, way, lanes, other]], axis=1)
            keys = k_all[block, :, :, lanes].reshape(2 * rows, LANES)
            score = jnp.dot(keys, queries, preferred_element_type=F32) * scale
            if diagonal:
                score = jnp.where(seen, score, -1e30)
            before = top[way, slot, head]
            peak = jnp.maximum(before, jnp.max(score, axis=0, keepdims=True))
            prob = jnp.exp2(score - peak).astype(BF16)
            weighed = (jnp.dot(v_all[block, 0, lanes], prob[:rows], preferred_element_type=F32)
                       + jnp.dot(v_all[block, 1, lanes], prob[rows:], preferred_element_type=F32))
            acc[way, slot, head] = acc[way, slot, head] * jnp.exp2(before - peak) + weighed
            top[way, slot, head] = peak

    def attend_ahead(offset, units):
        block = ring_to_chip((pos + offset) % RING)

        def queries_of(unit, carry):
            way, step = unit % 2, unit // 2
            at = scattered_block(way, step)

            @pl.when(block < at)
            def _():
                attend(way, step, at, block, False)

            return carry

        lax.fori_loop(0, units, queries_of, 0)

    def attended_by(way, step):
        at, slot = scattered_block(way, step), step % 2

        @pl.when(step >= 2)
        def _():
            fresh(way, slot)

            def body(earlier, carry):
                attend(way, slot, at, earlier, False)
                return carry

            lax.fori_loop(0, at, body, 0)

        @pl.when(step == 1)
        def _():
            def nearest(side, carry):
                block = ring_to_chip((pos + 1 + side * (RING - 2)) % RING)

                @pl.when(block < at)
                def _():
                    attend(way, slot, at, block, False)

                return carry

            lax.fori_loop(0, 2, nearest, 0)

        attend(way, slot, at, at, True)
        done = []
        for head in range(heads):
            sums = acc[way, slot, head]
            done.append((sums / sums[head_dim:head_dim + 1]).T.astype(BF16))
        return jnp.concatenate(done, axis=1)

    def both_sides(way, at):
        return jnp.concatenate([m_all[at, way, mine], m_all[at, way, other]], axis=0)

    def down_ahead(way):
        up = both_sides(way, scattered_block(way, 0))
        for low in range(0, depth, tile):
            cols = slice(low, low + tile)
            part_sum = jnp.dot(up, w_down[:, cols], preferred_element_type=F32)
            own[way, 0, :, cols] = part_sum[:half]
            own[way, 1, :, cols] = part_sum[half:]

    def contribute_first(way):
        attended = attended_by(way, 0)
        for low in range(0, depth, tile):
            cols = slice(low, low + tile)
            part_sum = jnp.dot(attended, w_o[:, cols], preferred_element_type=F32)
            own[way, 0, :, cols] = own[way, 0, :, cols] + part_sum[:half]
            given[way, 0, :, cols] = (own[way, 1, :, cols] + part_sum[half:]).astype(BF16)

    def contribute(way, step):
        at = scattered_block(way, step)
        attended = attended_by(way, step)
        up = both_sides(way, at)

        @pl.when(step >= 2)
        def _():
            pair_copy(way, step - 2).wait_send()

        for low in range(0, depth, tile):
            cols = slice(low, low + tile)
            part_sum = (jnp.dot(attended, w_o[:, cols], preferred_element_type=F32)
                        + jnp.dot(up, w_down[:, cols], preferred_element_type=F32))
            own[way, step % 2, :, cols] = part_sum[:half]
            given[way, step % 2, :, cols] = part_sum[half:].astype(BF16)
        pair_copy(way, step).start()

    def total(way, step, part):
        span = span_of(part)
        taken = pl.ds(pl.multiple_of(half + part * piece, piece), piece)
        return own[way, step % 2, span] + hbuf[way, step, taken].astype(F32) + hbuf[way, step, span].astype(F32)

    def tell(phase):
        for to in (right, left, partner):
            pl.semaphore_signal(ready.at[phase], inc=1, device_id={"tp": to}, device_id_type=MESH)

    barrier = call(right, left, partner)
    for copy in in_copies(0):
        copy.start()
    for g in range(3 * heads):
        staged[g, head_dim:] = jnp.zeros((LANES - head_dim, depth), BF16)
    for head in range(heads):
        w_o[head * LANES + head_dim:(head + 1) * LANES] = jnp.zeros((LANES - head_dim, depth), BF16)
    for wide, ref in ((b_up, bup_ref), (gain, gain_ref), (bias, bias_ref)):
        rows_f32 = ref[...].astype(F32)
        for layer in range(layers):
            wide[layer] = rows_f32[layer:layer + 1]
    rows_f32 = bo_ref[...].astype(F32) + bdown_ref[...].astype(F32)
    for layer in range(layers):
        b_sum[layer] = rows_f32[layer:layer + 1]
    column = lax.broadcasted_iota(jnp.int32, (1, 3 * width), 1)
    for layer in range(layers):
        b_qkv[layer] = jnp.where((column >= 2 * width) & (column % LANES == head_dim), 1.0, 0.0)
        for which, ref in enumerate((bq_ref, bk_ref, bv_ref)):
            heads_f32 = ref[layer].astype(F32)
            for head in range(heads):
                low = which * width + head * LANES
                b_qkv[layer, :, low:low + head_dim] = heads_f32[head:head + 1]
    out_ref[...] = x_ref[...]
    pl.semaphore_wait(barrier, 3)

    def layer_body(layer, carry):
        for copy in out_copies(layer):
            copy.start()
        for part in range(PARTS):
            for way in range(2):
                low = way * half + part * piece
                hbuf[way, 0, pl.ds(pl.multiple_of(core * half + part * piece, piece), piece)] = layer_norm(
                    out_ref[low:low + piece], gain[layer], bias[layer])
            if part == 0:
                @pl.when(layer > 0)
                def _():
                    pl.semaphore_wait(ready.at[3 * layer - 1], 3)

            for way in range(2):
                gather_copy(way, 0, part).start()
                share_copy(way, 0, part, core).start()

        for copy in in_copies(layer):
            copy.wait()
        for g in range(3 * heads):
            w_qkv[:, g * LANES:(g + 1) * LANES] = staged[g].T

        def arrive(event):
            step = 1 + event // 2
            for index in range(group):
                part = event % 2 * group + index
                for way in range(2):
                    gather_copy(way, step - 1, part).wait_recv()

                    @pl.when(step < RING - 1)
                    def _():
                        gather_copy(way, step, part).start()

                    share_copy(way, step, part, core).start()

        def first_units(unit, carry):
            project_kv(layer, unit, 0)
            project_rest(layer, unit, 0)
            return carry

        def events(event, carry):
            arrive(event)
            way, step = (event + 1) % 2, (event + 1) // 2
            project_kv(layer, way, step)
            project_rest(layer, way, step)

            @pl.when(event == 4)
            def _():
                for copy in out_copies(layer):
                    copy.wait()

            @pl.when((event >= 4) & (event < 6))
            def _():
                down_ahead(event - 4)

            @pl.when(event >= RING)
            def _():
                far, odd = (event - RING) // 2, event % 2
                attend_ahead((1 - odd) * (RING // 2 - far) + odd * (RING // 2 + far) * ((far + 1) // 2), 4)

            return carry

        def last_units(way, carry):
            project_kv(layer, way, RING - 1)
            return carry

        def nearest(side, carry):
            attend_ahead(1 + side * (RING - 2), 2)
            return carry

        for way in range(2):
            for slot in range(2):
                fresh(way, slot)
        lax.fori_loop(0, 2, first_units, 0)
        arrive(0)
        lax.fori_loop(1, 2 * RING - 3, events, 0)
        attend_ahead(RING - 2, 4)
        arrive(2 * RING - 3)
        lax.fori_loop(0, 2, last_units, 0)

        def drain_gather(step, carry):
            for way in range(2):
                for part in range(PARTS):
                    @pl.when(step < RING - 1)
                    def _():
                        gather_copy(way, step, part).wait_send()

                    share_copy(way, step, part, core).wait_send()
            return carry

        lax.fori_loop(0, RING, drain_gather, 0)
        tell(3 * layer)
        lax.fori_loop(0, 2, nearest, 0)
        for way in range(2):
            hbuf[way, 0, :half] = jnp.zeros((half, depth), BF16)

        def first_parts(way, carry):
            contribute_first(way)

            @pl.when(way == 0)
            def _():
                pl.semaphore_wait(ready.at[3 * layer], 3)

            pair_copy(way, 0).start()
            return carry

        def scatter_events(event, carry):
            step, second = event // 2, event % 2

            @pl.when(event == 2 * RING - 4)
            def _():
                pl.semaphore_wait(ready.at[3 * layer + 1], 3)

            for index in range(group):
                part = second * group + index
                for way in range(2):
                    if index == 0:
                        @pl.when(second == 0)
                        def _():
                            pair_copy(way, step).wait_recv()

                    @pl.when(step > 0)
                    def _():
                        scatter_copy(way, step - 1, part).wait_recv()

                    hbuf[way, step, span_of(part)] = total(way, step, part).astype(BF16)
                    scatter_copy(way, step, part).start()
            contribute(second, step + 1)

            @pl.when((event >= 1) & (event < 3))
            def _():
                project_rest(layer, event - 1, RING - 1)

            @pl.when(event == 2)
            def _():
                tell(3 * layer + 1)

                @pl.when(layer < layers - 1)
                def _():
                    for copy in in_copies(layer + 1):
                        copy.start()

            return carry

        lax.fori_loop(0, 2, first_parts, 0)
        lax.fori_loop(0, 2 * RING - 2, scatter_events, 0)
        for part in range(PARTS):
            for way in range(2):
                if part == 0:
                    pair_copy(way, RING - 1).wait_recv()
                scatter_copy(way, RING - 2, part).wait_recv()
                low = way * half + part * piece
                hidden = out_ref[low:low + piece].astype(F32) + total(way, RING - 1, part) + b_sum[layer]
                out_ref[low:low + piece] = hidden.astype(BF16)

        def drain_scatter(step, carry):
            for way in range(2):
                for part in range(PARTS):
                    scatter_copy(way, step, part).wait_send()
            return carry

        lax.fori_loop(0, RING - 1, drain_scatter, 0)
        for way in range(2):
            for step in (RING - 2, RING - 1):
                pair_copy(way, step).wait_send()

        @pl.when(layer < layers - 1)
        def _():
            tell(3 * layer + 2)

        return carry

    lax.fori_loop(0, layers, layer_body, 0)


def run_layers(x, w_q, w_k, w_v, w_o, w_up, w_down, vectors, tables):
    rows, depth = x.shape
    layers, heads, head_dim, _ = w_q.shape
    width, hidden_width = heads * LANES, w_up.shape[2]
    half = rows // 2
    vmem = pl.BlockSpec(memory_space=pltpu.VMEM)
    hbm = pl.BlockSpec(memory_space=pl.ANY)
    return pl.pallas_call(
        layers_kernel,
        out_shape=jax.ShapeDtypeStruct((rows, depth), BF16),
        in_specs=[vmem] + [hbm] * 6 + [vmem] * 12,
        out_specs=vmem,
        scratch_shapes=[
            pltpu.VMEM((layers, 1, 3 * width), F32),
            pltpu.VMEM((layers, 1, hidden_width), F32),
            pltpu.VMEM((layers, 1, depth), F32),
            pltpu.VMEM((layers, 1, depth), F32),
            pltpu.VMEM((layers, 1, depth), F32),
            pltpu.VMEM((2, RING, rows, depth), BF16),
            pltpu.VMEM((RING, 2, width, rows), BF16),
            pltpu.VMEM((RING, 2, rows, width), BF16),
            pltpu.VMEM((RING, 2, width, rows), BF16),
            pltpu.VMEM((RING, 2, rows, hidden_width), BF16),
            pltpu.VMEM((3 * heads, LANES, depth), BF16),
            pltpu.VMEM((depth, 3 * width), BF16),
            pltpu.VMEM((depth, hidden_width), BF16),
            pltpu.VMEM((width, depth), BF16),
            pltpu.VMEM((hidden_width, depth), BF16),
            pltpu.VMEM((2, 2, half, depth), BF16),
            pltpu.VMEM((2, 2, half, depth), F32),
            pltpu.VMEM((2, 2, heads, LANES, rows), F32),
            pltpu.VMEM((2, 2, heads, 1, rows), F32),
            pltpu.SemaphoreType.DMA((4 * heads + 2,)),
            pltpu.SemaphoreType.DMA((2, RING, PARTS)),
            pltpu.SemaphoreType.DMA((2, RING, PARTS)),
            pltpu.SemaphoreType.DMA((2, RING, PARTS)),
            pltpu.SemaphoreType.DMA((2, RING, PARTS)),
            pltpu.SemaphoreType.DMA((2, RING, PARTS)),
            pltpu.SemaphoreType.DMA((2, RING, PARTS)),
            pltpu.SemaphoreType.DMA((2, RING)),
            pltpu.SemaphoreType.DMA((2, RING)),
            pltpu.SemaphoreType.REGULAR((3 * layers,)),
        ],
        compiler_params=pltpu.CompilerParams(collective_id=0, has_side_effects=True, vmem_limit_bytes=VMEM_LIMIT),
        name="layers",
    )(x, w_q, w_k, w_v, w_o, w_up, w_down, *vectors, *tables)


def rotary_tables(rows):
    half = rows // 2
    way, core, row = jnp.meshgrid(jnp.arange(2), jnp.arange(2), jnp.arange(half), indexing="ij")
    offset = (core * rows + way * half + row).astype(F32).reshape(2, rows, 1)
    base = (jnp.arange(RING, dtype=F32) * (2 * rows)).reshape(RING, 1, 1)
    lane = jnp.arange(LANES)
    pair = (lane % (ROT_DIM // 2)).astype(F32)
    inv_freq = jnp.where(lane < ROT_DIM, 1.0 / (ROPE_BASE ** (pair * (2.0 / ROT_DIM))), 0.0)
    return jnp.cos(base * inv_freq), jnp.sin(base * inv_freq), jnp.cos(offset * inv_freq), jnp.sin(offset * inv_freq)


def solution(mesh):
    head_spec = P(None, None, "tp", None)
    head_bias_spec = P(None, "tp", None)
    in_specs = (P("dp", "tp", None), P(), P(), head_spec, head_bias_spec, head_spec, head_bias_spec, head_spec, head_bias_spec,
                P(None, "tp", None, None), P(), P(None, None, "tp"), P(None, "tp"), P(None, "tp", None), P())

    def local_program(x_loc, ln_gain, ln_bias, w_q, b_q, w_k, b_k, w_v, b_v, w_o, b_o, w_up, b_up, w_down, b_down):
        def heads_first(weight):
            return jnp.transpose(weight, (0, 2, 3, 1))

        out = run_layers(x_loc[0], heads_first(w_q), heads_first(w_k), heads_first(w_v), w_o, w_up, w_down,
                         (b_q, b_k, b_v, b_up, b_o, b_down, ln_gain, ln_bias), rotary_tables(x_loc.shape[1]))
        return out[None]

    return jax.shard_map(local_program, mesh=mesh, in_specs=in_specs, out_specs=P("dp", "tp", None), check_vma=False)
```

```python
import functools

import jax
import jax.numpy as jnp
from jax import lax
from jax.experimental import pallas as pl
from jax.experimental.pallas import tpu as pltpu
from jax.sharding import PartitionSpec as P

ROT_DIM = 32
ROPE_BASE = 10000.0
LN_EPS = 1e-5
LANES = 128
RING = 8
PARTS = 2
LOG2_E = 1.4426950408889634
MESH = pl.DeviceIdType.MESH
VMEM_LIMIT = 67043328
F32 = jnp.float32
BF16 = jnp.bfloat16


def ring_to_chip(pos):
    y = ((pos + 3) // 4) % 2
    z = y * (pos - 1) + (1 - y) * ((RING - pos) % RING)
    return 2 * z + y


def chip_to_ring(chip):
    y = chip % 2
    z = chip // 2
    return y * (z + 1) + (1 - y) * ((RING - z) % RING)


def place():
    me = lax.axis_index("tp")
    core = me % 2
    chip = me // 2
    pos = chip_to_ring(chip)
    right = 2 * ring_to_chip((pos + 1) % RING) + core
    left = 2 * ring_to_chip((pos + RING - 1) % RING) + core
    partner = 2 * chip + (1 - core)
    return core, chip, pos, right, left, partner


def call(right, left, partner):
    barrier = pltpu.get_barrier_semaphore()
    for other in (right, left, partner):
        pl.semaphore_signal(barrier, inc=1, device_id={"tp": other}, device_id_type=MESH)
    return barrier


def layer_norm(hidden, gain, bias):
    x_f32 = hidden.astype(F32)
    mean = jnp.mean(x_f32, axis=-1, keepdims=True)
    centered = x_f32 - mean
    variance = jnp.mean(centered * centered, axis=-1, keepdims=True)
    return (centered * lax.rsqrt(variance + LN_EPS) * gain + bias).astype(BF16)


def layers_kernel(x_hbm, wq_hbm, wk_hbm, wv_hbm, wo_hbm, wup_hbm, wdown_hbm, bq_ref, bk_ref, bv_ref, bup_ref, bo_ref, bdown_ref,
                  gain_ref, bias_ref, freq_ref, out_hbm,
                  kept, base_cos, base_sin, step_cos, step_sin, b_qkv, b_up, b_sum, gain, bias, hbuf, q_all, k_all, v_all, m_all, staged, w_qkv, w_up, w_o, w_down, given, own, acc, top,
                  weight_sem, gather_send, gather_recv, share_send, share_recv,
                  scatter_send, scatter_recv, pair_send, pair_recv, ready, edge_sem):
    layers, heads, head_dim, depth = wq_hbm.shape
    rows = x_hbm.shape[0]
    half = rows // 2
    piece = half // PARTS
    group = PARTS // 2
    width = heads * LANES
    tile = next(t for t in (512, 256, 128) if depth % t == 0)
    scale = head_dim ** -0.5 * LOG2_E
    core, chip, pos, right, left, partner = place()
    mine, other = pl.ds(pl.multiple_of(core * half, half), half), pl.ds(pl.multiple_of((1 - core) * half, half), half)

    def span_of(part):
        return pl.ds(pl.multiple_of(part * piece, piece), piece)

    def remote(src, dst, send_sem, recv_sem, to):
        return pltpu.make_async_remote_copy(src_ref=src, dst_ref=dst, send_sem=send_sem, recv_sem=recv_sem,
                                            device_id={"tp": to}, device_id_type=MESH)

    def next_of(way):
        return right if way == 0 else left

    def in_copies(layer):
        copies = [pltpu.make_async_copy(hbm.at[layer, head], staged.at[which * heads + head, pl.ds(0, head_dim)],
                                        weight_sem.at[which * heads + head])
                  for which, hbm in enumerate((wq_hbm, wk_hbm, wv_hbm)) for head in range(heads)]
        return copies + [pltpu.make_async_copy(wup_hbm.at[layer], w_up, weight_sem.at[3 * heads])]

    def out_copies(layer):
        copies = [pltpu.make_async_copy(wo_hbm.at[layer, head], w_o.at[pl.ds(head * LANES, head_dim)],
                                        weight_sem.at[3 * heads + 1 + head]) for head in range(heads)]
        return copies + [pltpu.make_async_copy(wdown_hbm.at[layer], w_down, weight_sem.at[4 * heads + 1])]

    def gathered_block(way, step):
        return ring_to_chip((pos + (1 - way) * (RING - step) + way * step) % RING)

    def gather_rows(way, step, part, side):
        return hbuf.at[way, step, pl.ds(pl.multiple_of(side * half + part * piece, piece), piece)]

    def gather_copy(way, step, part):
        return remote(gather_rows(way, step, part, core), gather_rows(way, step + 1, part, core),
                      gather_send.at[way, step, part], gather_recv.at[way, step, part], next_of(way))

    def share_copy(way, step, part, side):
        ref = gather_rows(way, step, part, side)
        return remote(ref, ref, share_send.at[way, step, part], share_recv.at[way, step, part], partner)

    def rotate(value, cosine, sine):
        lane = lax.broadcasted_iota(jnp.int32, value.shape, 1)
        swapped = jnp.where(lane < ROT_DIM // 2, pltpu.roll(value, LANES - ROT_DIM // 2, 1), pltpu.roll(value, ROT_DIM // 2, 1))
        return value * cosine + swapped * sine

    def turning(way, at):
        cos_0, sin_0, cos_1, sin_1 = base_cos[at], base_sin[at], step_cos[way], step_sin[way]
        lane = lax.broadcasted_iota(jnp.int32, (1, LANES), 1)
        sign = jnp.where(lane < ROT_DIM // 2, -1.0, 1.0)
        return cos_0 * cos_1 - sin_0 * sin_1, (sin_0 * cos_1 + cos_0 * sin_1) * sign

    def project(layer, way, step, which):
        cols = slice(which * width, (which + 1) * width)
        return jnp.dot(hbuf[way, step], w_qkv[:, cols], preferred_element_type=F32) + b_qkv[layer, :, cols]

    def project_kv(layer, way, step):
        for part in range(PARTS):
            share_copy(way, step, part, 1 - core).wait_recv()
        at = gathered_block(way, step)
        cosine, sine = turning(way, at)
        keys, values = project(layer, way, step, 1), project(layer, way, step, 2)
        for head in range(heads):
            lanes = slice(head * LANES, (head + 1) * LANES)
            k_all[at, way, :, lanes] = rotate(keys[:, lanes], cosine, sine).astype(BF16)
            v_all[at, way, lanes] = values[:, lanes].T.astype(BF16)

    def project_rest(layer, way, step):
        at = gathered_block(way, step)
        cosine, sine = turning(way, at)
        queries = project(layer, way, step, 0)
        for head in range(heads):
            lanes = slice(head * LANES, (head + 1) * LANES)
            q_all[at, way, lanes] = rotate(queries[:, lanes], cosine, sine).T.astype(BF16)
        up = jnp.dot(hbuf[way, step], w_up[...], preferred_element_type=F32) + b_up[layer]
        m_all[at, way] = jax.nn.gelu(up, approximate=True).astype(BF16)

    def scattered_block(way, step):
        return ring_to_chip((pos + (1 - way) * (2 * RING - 1 - step) + way * (1 + step)) % RING)

    def scatter_copy(way, step, part):
        span = span_of(part)
        return remote(hbuf.at[way, step, span], hbuf.at[way, step + 1, span],
                      scatter_send.at[way, step, part], scatter_recv.at[way, step, part], next_of(way))

    def pair_copy(way, step):
        return remote(given.at[way, step % 2], hbuf.at[way, step, pl.ds(half, half)],
                      pair_send.at[way, step], pair_recv.at[way, step], partner)

    def fresh(way, slot):
        acc[way, slot] = jnp.zeros((heads, LANES, rows), F32)
        top[way, slot] = jnp.full((heads, 1, rows), -1e30, F32)

    def attend(way, slot, at, block, diagonal):
        if diagonal:
            key = lax.broadcasted_iota(jnp.int32, (2 * rows, 1), 0)
            key_pos = ((key // half) % 2) * (2 * half) + (key // rows) * half + key % half
            query = lax.broadcasted_iota(jnp.int32, (1, rows), 1)
            query_pos = ((query // half + core) % 2) * (2 * half) + way * half + query % half
            seen = query_pos >= key_pos
        for head in range(heads):
            lanes = slice(head * LANES, (head + 1) * LANES)
            queries = jnp.concatenate([q_all[at, way, lanes, mine], q_all[at, way, lanes, other]], axis=1)
            keys = k_all[block, :, :, lanes].reshape(2 * rows, LANES)
            score = jnp.dot(keys, queries, preferred_element_type=F32) * scale
            if diagonal:
                score = jnp.where(seen, score, -1e30)
            before = top[way, slot, head]
            peak = jnp.maximum(before, jnp.max(score, axis=0, keepdims=True))
            prob = jnp.exp2(score - peak).astype(BF16)
            weighed = (jnp.dot(v_all[block, 0, lanes], prob[:rows], preferred_element_type=F32)
                       + jnp.dot(v_all[block, 1, lanes], prob[rows:], preferred_element_type=F32))
            acc[way, slot, head] = acc[way, slot, head] * jnp.exp2(before - peak) + weighed
            top[way, slot, head] = peak

    def attend_ahead(offset, units):
        block = ring_to_chip((pos + offset) % RING)

        def queries_of(unit, carry):
            way, step = unit % 2, unit // 2
            at = scattered_block(way, step)

            @pl.when(block < at)
            def _():
                attend(way, step, at, block, False)

            return carry

        lax.fori_loop(0, units, queries_of, 0)

    def attended_by(way, step):
        at, slot = scattered_block(way, step), step % 2

        @pl.when(step >= 2)
        def _():
            fresh(way, slot)

            def body(earlier, carry):
                attend(way, slot, at, earlier, False)
                return carry

            lax.fori_loop(0, at, body, 0)

        @pl.when(step == 1)
        def _():
            def nearest(side, carry):
                block = ring_to_chip((pos + 1 + side * (RING - 2)) % RING)

                @pl.when(block < at)
                def _():
                    attend(way, slot, at, block, False)

                return carry

            lax.fori_loop(0, 2, nearest, 0)

        attend(way, slot, at, at, True)
        done = []
        for head in range(heads):
            sums = acc[way, slot, head]
            done.append((sums / sums[head_dim:head_dim + 1]).T.astype(BF16))
        return jnp.concatenate(done, axis=1)

    def both_sides(way, at):
        return jnp.concatenate([m_all[at, way, mine], m_all[at, way, other]], axis=0)

    def down_ahead(way):
        up = both_sides(way, scattered_block(way, 0))
        for low in range(0, depth, tile):
            cols = slice(low, low + tile)
            part_sum = jnp.dot(up, w_down[:, cols], preferred_element_type=F32)
            own[way, 0, :, cols] = part_sum[:half]
            own[way, 1, :, cols] = part_sum[half:]

    def contribute_first(way):
        attended = attended_by(way, 0)
        for low in range(0, depth, tile):
            cols = slice(low, low + tile)
            part_sum = jnp.dot(attended, w_o[:, cols], preferred_element_type=F32)
            own[way, 0, :, cols] = own[way, 0, :, cols] + part_sum[:half]
            given[way, 0, :, cols] = (own[way, 1, :, cols] + part_sum[half:]).astype(BF16)

    def contribute(way, step):
        at = scattered_block(way, step)
        attended = attended_by(way, step)
        up = both_sides(way, at)

        @pl.when(step >= 2)
        def _():
            pair_copy(way, step - 2).wait_send()

        for low in range(0, depth, tile):
            cols = slice(low, low + tile)
            part_sum = (jnp.dot(attended, w_o[:, cols], preferred_element_type=F32)
                        + jnp.dot(up, w_down[:, cols], preferred_element_type=F32))
            own[way, step % 2, :, cols] = part_sum[:half]
            given[way, step % 2, :, cols] = part_sum[half:].astype(BF16)
        pair_copy(way, step).start()

    def total(way, step, part):
        span = span_of(part)
        taken = pl.ds(pl.multiple_of(half + part * piece, piece), piece)
        return own[way, step % 2, span] + hbuf[way, step, taken].astype(F32) + hbuf[way, step, span].astype(F32)

    def out_copy(way, part):
        span = pl.ds(way * half + part * piece, piece)
        return pltpu.make_async_copy(kept.at[span], out_hbm.at[span], edge_sem.at[1 + way * PARTS + part])

    def tell(phase):
        for to in (right, left, partner):
            pl.semaphore_signal(ready.at[phase], inc=1, device_id={"tp": to}, device_id_type=MESH)

    x_copy = pltpu.make_async_copy(x_hbm, kept, edge_sem.at[0])
    x_copy.start()
    barrier = call(right, left, partner)
    for copy in in_copies(0):
        copy.start()
    for g in range(3 * heads):
        staged[g, head_dim:] = jnp.zeros((LANES - head_dim, depth), BF16)
    for head in range(heads):
        w_o[head * LANES + head_dim:(head + 1) * LANES] = jnp.zeros((LANES - head_dim, depth), BF16)
    for wide, ref in ((b_up, bup_ref), (gain, gain_ref), (bias, bias_ref)):
        rows_f32 = ref[...].astype(F32)
        for layer in range(layers):
            wide[layer] = rows_f32[layer:layer + 1]
    rows_f32 = bo_ref[...].astype(F32) + bdown_ref[...].astype(F32)
    for layer in range(layers):
        b_sum[layer] = rows_f32[layer:layer + 1]
    column = lax.broadcasted_iota(jnp.int32, (1, 3 * width), 1)
    for layer in range(layers):
        b_qkv[layer] = jnp.where((column >= 2 * width) & (column % LANES == head_dim), 1.0, 0.0)
        for which, ref in enumerate((bq_ref, bk_ref, bv_ref)):
            heads_f32 = ref[layer].astype(F32)
            for head in range(heads):
                low = which * width + head * LANES
                b_qkv[layer, :, low:low + head_dim] = heads_f32[head:head + 1]
    x_copy.wait()
    pl.semaphore_wait(barrier, 3)

    def layer_body(layer, carry):
        for copy in out_copies(layer):
            copy.start()
        for part in range(PARTS):
            for way in range(2):
                low = way * half + part * piece
                hbuf[way, 0, pl.ds(pl.multiple_of(core * half + part * piece, piece), piece)] = layer_norm(
                    kept[low:low + piece], gain[layer], bias[layer])
            if part == 0:
                @pl.when(layer > 0)
                def _():
                    pl.semaphore_wait(ready.at[3 * layer - 1], 3)

            for way in range(2):
                gather_copy(way, 0, part).start()
                share_copy(way, 0, part, core).start()

        @pl.when(layer == 0)
        def _():
            chips = lax.broadcasted_iota(jnp.int32, (RING, 1), 0) * (2 * rows)
            angle = chips.astype(F32) * freq_ref[...]
            cosine, sine = jnp.cos(angle), jnp.sin(angle)
            for at in range(RING):
                base_cos[at] = cosine[at:at + 1]
                base_sin[at] = sine[at:at + 1]
            row = lax.broadcasted_iota(jnp.int32, (rows, 1), 0)
            for way in range(2):
                offset = (row // half) * rows + way * half + row % half
                angle = offset.astype(F32) * freq_ref[...]
                step_cos[way] = jnp.cos(angle)
                step_sin[way] = jnp.sin(angle)

        for copy in in_copies(layer):
            copy.wait()
        for g in range(3 * heads):
            w_qkv[:, g * LANES:(g + 1) * LANES] = staged[g].T

        def arrive(event):
            step = 1 + event // 2
            for index in range(group):
                part = event % 2 * group + index
                for way in range(2):
                    gather_copy(way, step - 1, part).wait_recv()

                    @pl.when(step < RING - 1)
                    def _():
                        gather_copy(way, step, part).start()

                    share_copy(way, step, part, core).start()

        def first_units(unit, carry):
            project_kv(layer, unit, 0)
            project_rest(layer, unit, 0)
            return carry

        def events(event, carry):
            arrive(event)
            way, step = (event + 1) % 2, (event + 1) // 2
            project_kv(layer, way, step)
            project_rest(layer, way, step)

            @pl.when(event == 4)
            def _():
                for copy in out_copies(layer):
                    copy.wait()

            @pl.when((event >= 4) & (event < 6))
            def _():
                down_ahead(event - 4)

            @pl.when(event >= RING)
            def _():
                far, odd = (event - RING) // 2, event % 2
                attend_ahead((1 - odd) * (RING // 2 - far) + odd * (RING // 2 + far) * ((far + 1) // 2), 4)

            return carry

        def last_units(way, carry):
            project_kv(layer, way, RING - 1)
            return carry

        def nearest(side, carry):
            attend_ahead(1 + side * (RING - 2), 2)
            return carry

        for way in range(2):
            for slot in range(2):
                fresh(way, slot)
        lax.fori_loop(0, 2, first_units, 0)
        arrive(0)
        lax.fori_loop(1, 2 * RING - 3, events, 0)
        attend_ahead(RING - 2, 4)
        arrive(2 * RING - 3)
        lax.fori_loop(0, 2, last_units, 0)

        def drain_gather(step, carry):
            for way in range(2):
                for part in range(PARTS):
                    @pl.when(step < RING - 1)
                    def _():
                        gather_copy(way, step, part).wait_send()

                    share_copy(way, step, part, core).wait_send()
            return carry

        lax.fori_loop(0, RING, drain_gather, 0)
        tell(3 * layer)
        lax.fori_loop(0, 2, nearest, 0)
        for way in range(2):
            hbuf[way, 0, :half] = jnp.zeros((half, depth), BF16)

        def first_parts(way, carry):
            contribute_first(way)

            @pl.when(way == 0)
            def _():
                pl.semaphore_wait(ready.at[3 * layer], 3)

            pair_copy(way, 0).start()
            return carry

        def scatter_events(event, carry):
            step, second = event // 2, event % 2

            @pl.when(event == 2 * RING - 4)
            def _():
                pl.semaphore_wait(ready.at[3 * layer + 1], 3)

            for index in range(group):
                part = second * group + index
                for way in range(2):
                    if index == 0:
                        @pl.when(second == 0)
                        def _():
                            pair_copy(way, step).wait_recv()

                    @pl.when(step > 0)
                    def _():
                        scatter_copy(way, step - 1, part).wait_recv()

                    hbuf[way, step, span_of(part)] = total(way, step, part).astype(BF16)
                    scatter_copy(way, step, part).start()
            contribute(second, step + 1)

            @pl.when((event >= 1) & (event < 3))
            def _():
                project_rest(layer, event - 1, RING - 1)

            @pl.when(event == 2)
            def _():
                tell(3 * layer + 1)

                @pl.when(layer < layers - 1)
                def _():
                    for copy in in_copies(layer + 1):
                        copy.start()

            return carry

        lax.fori_loop(0, 2, first_parts, 0)
        lax.fori_loop(0, 2 * RING - 2, scatter_events, 0)
        for part in range(PARTS):
            for way in range(2):
                if part == 0:
                    pair_copy(way, RING - 1).wait_recv()
                scatter_copy(way, RING - 2, part).wait_recv()
                low = way * half + part * piece
                hidden = kept[low:low + piece].astype(F32) + total(way, RING - 1, part) + b_sum[layer]
                kept[low:low + piece] = hidden.astype(BF16)

                @pl.when(layer == layers - 1)
                def _():
                    out_copy(way, part).start()


        def drain_scatter(step, carry):
            for way in range(2):
                for part in range(PARTS):
                    scatter_copy(way, step, part).wait_send()
            return carry

        lax.fori_loop(0, RING - 1, drain_scatter, 0)
        for way in range(2):
            for step in (RING - 2, RING - 1):
                pair_copy(way, step).wait_send()

        @pl.when(layer < layers - 1)
        def _():
            tell(3 * layer + 2)

        return carry

    lax.fori_loop(0, layers, layer_body, 0)
    for part in range(PARTS):
        for way in range(2):
            out_copy(way, part).wait()


def run_layers(x, w_q, w_k, w_v, w_o, w_up, w_down, vectors, freq):
    rows, depth = x.shape
    layers, heads, head_dim, _ = w_q.shape
    width, hidden_width = heads * LANES, w_up.shape[2]
    half = rows // 2
    vmem = pl.BlockSpec(memory_space=pltpu.VMEM)
    hbm = pl.BlockSpec(memory_space=pl.ANY)
    return pl.pallas_call(
        layers_kernel,
        out_shape=jax.ShapeDtypeStruct((rows, depth), BF16),
        in_specs=[hbm] * 7 + [vmem] * 9,
        out_specs=hbm,
        scratch_shapes=[
            pltpu.VMEM((rows, depth), BF16),
            pltpu.VMEM((RING, 1, LANES), F32),
            pltpu.VMEM((RING, 1, LANES), F32),
            pltpu.VMEM((2, rows, LANES), F32),
            pltpu.VMEM((2, rows, LANES), F32),
            pltpu.VMEM((layers, 1, 3 * width), F32),
            pltpu.VMEM((layers, 1, hidden_width), F32),
            pltpu.VMEM((layers, 1, depth), F32),
            pltpu.VMEM((layers, 1, depth), F32),
            pltpu.VMEM((layers, 1, depth), F32),
            pltpu.VMEM((2, RING, rows, depth), BF16),
            pltpu.VMEM((RING, 2, width, rows), BF16),
            pltpu.VMEM((RING, 2, rows, width), BF16),
            pltpu.VMEM((RING, 2, width, rows), BF16),
            pltpu.VMEM((RING, 2, rows, hidden_width), BF16),
            pltpu.VMEM((3 * heads, LANES, depth), BF16),
            pltpu.VMEM((depth, 3 * width), BF16),
            pltpu.VMEM((depth, hidden_width), BF16),
            pltpu.VMEM((width, depth), BF16),
            pltpu.VMEM((hidden_width, depth), BF16),
            pltpu.VMEM((2, 2, half, depth), BF16),
            pltpu.VMEM((2, 2, half, depth), F32),
            pltpu.VMEM((2, 2, heads, LANES, rows), F32),
            pltpu.VMEM((2, 2, heads, 1, rows), F32),
            pltpu.SemaphoreType.DMA((4 * heads + 2,)),
            pltpu.SemaphoreType.DMA((2, RING, PARTS)),
            pltpu.SemaphoreType.DMA((2, RING, PARTS)),
            pltpu.SemaphoreType.DMA((2, RING, PARTS)),
            pltpu.SemaphoreType.DMA((2, RING, PARTS)),
            pltpu.SemaphoreType.DMA((2, RING, PARTS)),
            pltpu.SemaphoreType.DMA((2, RING, PARTS)),
            pltpu.SemaphoreType.DMA((2, RING)),
            pltpu.SemaphoreType.DMA((2, RING)),
            pltpu.SemaphoreType.REGULAR((3 * layers,)),
            pltpu.SemaphoreType.DMA((1 + 2 * PARTS,)),
        ],
        compiler_params=pltpu.CompilerParams(collective_id=0, has_side_effects=True, vmem_limit_bytes=VMEM_LIMIT),
        name="layers",
    )(x, w_q, w_k, w_v, w_o, w_up, w_down, *vectors, freq)


def rotary_frequencies():
    lane = jnp.arange(LANES)
    pair = (lane % (ROT_DIM // 2)).astype(F32)
    return jnp.where(lane < ROT_DIM, 1.0 / (ROPE_BASE ** (pair * (2.0 / ROT_DIM))), 0.0).reshape(1, LANES)


def solution(mesh):
    head_spec = P(None, None, "tp", None)
    head_bias_spec = P(None, "tp", None)
    in_specs = (P("dp", "tp", None), P(), P(), head_spec, head_bias_spec, head_spec, head_bias_spec, head_spec, head_bias_spec,
                P(None, "tp", None, None), P(), P(None, None, "tp"), P(None, "tp"), P(None, "tp", None), P())

    def local_program(x_loc, ln_gain, ln_bias, w_q, b_q, w_k, b_k, w_v, b_v, w_o, b_o, w_up, b_up, w_down, b_down):
        def heads_first(weight):
            return jnp.transpose(weight, (0, 2, 3, 1))

        out = run_layers(x_loc[0], heads_first(w_q), heads_first(w_k), heads_first(w_v), w_o, w_up, w_down,
                         (b_q, b_k, b_v, b_up, b_o, b_down, ln_gain, ln_bias), rotary_frequencies())
        return out[None]

    return jax.shard_map(local_program, mesh=mesh, in_specs=in_specs, out_specs=P("dp", "tp", None), check_vma=False)
```

```python
import functools

import jax
import jax.numpy as jnp
from jax import lax
from jax.experimental import pallas as pl
from jax.experimental.pallas import tpu as pltpu
from jax.sharding import PartitionSpec as P

ROT_DIM = 32
ROPE_BASE = 10000.0
LN_EPS = 1e-5
LANES = 128
RING = 8
PARTS = 2
LOG2_E = 1.4426950408889634
MESH = pl.DeviceIdType.MESH
VMEM_LIMIT = 67043328
F32 = jnp.float32
BF16 = jnp.bfloat16


def ring_to_chip(pos):
    y = ((pos + 3) // 4) % 2
    z = y * (pos - 1) + (1 - y) * ((RING - pos) % RING)
    return 2 * z + y


def chip_to_ring(chip):
    y = chip % 2
    z = chip // 2
    return y * (z + 1) + (1 - y) * ((RING - z) % RING)


def place():
    me = lax.axis_index("tp")
    core = me % 2
    chip = me // 2
    pos = chip_to_ring(chip)
    right = 2 * ring_to_chip((pos + 1) % RING) + core
    left = 2 * ring_to_chip((pos + RING - 1) % RING) + core
    partner = 2 * chip + (1 - core)
    return core, chip, pos, right, left, partner


def call(right, left, partner):
    barrier = pltpu.get_barrier_semaphore()
    for other in (right, left, partner):
        pl.semaphore_signal(barrier, inc=1, device_id={"tp": other}, device_id_type=MESH)
    return barrier


def layer_norm(hidden, gain, bias):
    x_f32 = hidden.astype(F32)
    mean = jnp.mean(x_f32, axis=-1, keepdims=True)
    centered = x_f32 - mean
    variance = jnp.mean(centered * centered, axis=-1, keepdims=True)
    return (centered * lax.rsqrt(variance + LN_EPS) * gain + bias).astype(BF16)


def layers_kernel(x_hbm, wq_hbm, wk_hbm, wv_hbm, wo_hbm, wup_hbm, wdown_hbm, bq_ref, bk_ref, bv_ref, bup_ref, bo_ref, bdown_ref,
                  gain_ref, bias_ref, freq_ref, out_hbm,
                  kept, base_cos, base_sin, step_cos, step_sin, b_qkv, b_up, b_sum, gain, bias, hbuf, q_all, k_all, v_all, m_all, staged, w_qkv, w_up, w_o, w_down, given, own, acc, top,
                  weight_sem, gather_send, gather_recv, share_send, share_recv,
                  scatter_send, scatter_recv, pair_send, pair_recv, ready, edge_sem):
    layers, heads, head_dim, depth = wq_hbm.shape
    rows = x_hbm.shape[0]
    half = rows // 2
    piece = half // PARTS
    group = PARTS // 2
    width = heads * LANES
    tile = next(t for t in (512, 256, 128) if depth % t == 0)
    scale = head_dim ** -0.5 * LOG2_E
    core, chip, pos, right, left, partner = place()
    mine, other = pl.ds(pl.multiple_of(core * half, half), half), pl.ds(pl.multiple_of((1 - core) * half, half), half)

    def span_of(part):
        return pl.ds(pl.multiple_of(part * piece, piece), piece)

    def remote(src, dst, send_sem, recv_sem, to):
        return pltpu.make_async_remote_copy(src_ref=src, dst_ref=dst, send_sem=send_sem, recv_sem=recv_sem,
                                            device_id={"tp": to}, device_id_type=MESH)

    def next_of(way):
        return right if way == 0 else left

    def in_copies(layer):
        copies = [pltpu.make_async_copy(hbm.at[layer, head], staged.at[which * heads + head, pl.ds(0, head_dim)],
                                        weight_sem.at[which * heads + head])
                  for which, hbm in enumerate((wq_hbm, wk_hbm, wv_hbm)) for head in range(heads)]
        return copies + [pltpu.make_async_copy(wup_hbm.at[layer], w_up, weight_sem.at[3 * heads])]

    def out_copies(layer):
        copies = [pltpu.make_async_copy(wo_hbm.at[layer, head], w_o.at[pl.ds(head * LANES, head_dim)],
                                        weight_sem.at[3 * heads + 1 + head]) for head in range(heads)]
        return copies + [pltpu.make_async_copy(wdown_hbm.at[layer], w_down, weight_sem.at[4 * heads + 1])]

    def gathered_block(way, step):
        return ring_to_chip((pos + (1 - way) * (RING - step) + way * step) % RING)

    def gather_rows(way, step, part, side):
        return hbuf.at[way, step, pl.ds(pl.multiple_of(side * half + part * piece, piece), piece)]

    def gather_copy(way, step, part):
        return remote(gather_rows(way, step, part, core), gather_rows(way, step + 1, part, core),
                      gather_send.at[way, step, part], gather_recv.at[way, step, part], next_of(way))

    def share_copy(way, step, part, side):
        ref = gather_rows(way, step, part, side)
        return remote(ref, ref, share_send.at[way, step, part], share_recv.at[way, step, part], partner)

    def rotate(value, cosine, sine):
        lane = lax.broadcasted_iota(jnp.int32, value.shape, 1)
        swapped = jnp.where(lane < ROT_DIM // 2, pltpu.roll(value, LANES - ROT_DIM // 2, 1), pltpu.roll(value, ROT_DIM // 2, 1))
        return value * cosine + swapped * sine

    def turning(way, at):
        cos_0, sin_0, cos_1, sin_1 = base_cos[at], base_sin[at], step_cos[way], step_sin[way]
        lane = lax.broadcasted_iota(jnp.int32, (1, LANES), 1)
        sign = jnp.where(lane < ROT_DIM // 2, -1.0, 1.0)
        return cos_0 * cos_1 - sin_0 * sin_1, (sin_0 * cos_1 + cos_0 * sin_1) * sign

    def project(layer, way, step, which):
        cols = slice(which * width, (which + 1) * width)
        return jnp.dot(hbuf[way, step], w_qkv[:, cols], preferred_element_type=F32) + b_qkv[layer, :, cols]

    def project_kv(layer, way, step):
        for part in range(PARTS):
            share_copy(way, step, part, 1 - core).wait_recv()
        at = gathered_block(way, step)
        cosine, sine = turning(way, at)
        keys, values = project(layer, way, step, 1), project(layer, way, step, 2)
        for head in range(heads):
            lanes = slice(head * LANES, (head + 1) * LANES)
            k_all[at, way, :, lanes] = rotate(keys[:, lanes], cosine, sine).astype(BF16)
            v_all[at, way, lanes] = values[:, lanes].T.astype(BF16)

    def project_rest(layer, way, step):
        at = gathered_block(way, step)
        cosine, sine = turning(way, at)
        queries = project(layer, way, step, 0)
        for head in range(heads):
            lanes = slice(head * LANES, (head + 1) * LANES)
            q_all[at, way, lanes] = rotate(queries[:, lanes], cosine, sine).T.astype(BF16)
        up = jnp.dot(hbuf[way, step], w_up[...], preferred_element_type=F32) + b_up[layer]
        m_all[at, way] = jax.nn.gelu(up, approximate=True).astype(BF16)

    def scattered_block(way, step):
        return ring_to_chip((pos + (1 - way) * (2 * RING - 1 - step) + way * (1 + step)) % RING)

    def scatter_copy(way, step, part):
        span = span_of(part)
        return remote(hbuf.at[way, step, span], hbuf.at[way, step + 1, span],
                      scatter_send.at[way, step, part], scatter_recv.at[way, step, part], next_of(way))

    def pair_copy(way, step):
        return remote(given.at[way, step % 2], hbuf.at[way, step, pl.ds(half, half)],
                      pair_send.at[way, step], pair_recv.at[way, step], partner)

    def fresh(way, slot):
        acc[way, slot] = jnp.zeros((heads, LANES, rows), F32)
        top[way, slot] = jnp.full((heads, 1, rows), -1e30, F32)

    def attend(way, slot, at, block, diagonal):
        if diagonal:
            key = lax.broadcasted_iota(jnp.int32, (2 * rows, 1), 0)
            key_pos = ((key // half) % 2) * (2 * half) + (key // rows) * half + key % half
            query = lax.broadcasted_iota(jnp.int32, (1, rows), 1)
            query_pos = ((query // half + core) % 2) * (2 * half) + way * half + query % half
            seen = query_pos >= key_pos
        for head in range(heads):
            lanes = slice(head * LANES, (head + 1) * LANES)
            queries = jnp.concatenate([q_all[at, way, lanes, mine], q_all[at, way, lanes, other]], axis=1)
            keys = k_all[block, :, :, lanes].reshape(2 * rows, LANES)
            score = jnp.dot(keys, queries, preferred_element_type=F32) * scale
            if diagonal:
                score = jnp.where(seen, score, -1e30)
            before = top[way, slot, head]
            peak = jnp.maximum(before, jnp.max(score, axis=0, keepdims=True))
            prob = jnp.exp2(score - peak).astype(BF16)
            weighed = (jnp.dot(v_all[block, 0, lanes], prob[:rows], preferred_element_type=F32)
                       + jnp.dot(v_all[block, 1, lanes], prob[rows:], preferred_element_type=F32))
            acc[way, slot, head] = acc[way, slot, head] * jnp.exp2(before - peak) + weighed
            top[way, slot, head] = peak

    def attend_ahead(offset, units):
        block = ring_to_chip((pos + offset) % RING)

        def queries_of(unit, carry):
            way, step = unit % 2, unit // 2
            at = scattered_block(way, step)

            @pl.when(block < at)
            def _():
                attend(way, step, at, block, False)

            return carry

        lax.fori_loop(0, units, queries_of, 0)

    def attended_by(way, step):
        at, slot = scattered_block(way, step), step % 2

        @pl.when(step >= 2)
        def _():
            fresh(way, slot)

            def body(earlier, carry):
                attend(way, slot, at, earlier, False)
                return carry

            lax.fori_loop(0, at, body, 0)

        @pl.when(step == 1)
        def _():
            def nearest(side, carry):
                block = ring_to_chip((pos + 1 + side * (RING - 2)) % RING)

                @pl.when(block < at)
                def _():
                    attend(way, slot, at, block, False)

                return carry

            lax.fori_loop(0, 2, nearest, 0)

        attend(way, slot, at, at, True)
        done = []
        for head in range(heads):
            sums = acc[way, slot, head]
            done.append((sums / sums[head_dim:head_dim + 1]).T.astype(BF16))
        return jnp.concatenate(done, axis=1)

    def both_sides(way, at):
        return jnp.concatenate([m_all[at, way, mine], m_all[at, way, other]], axis=0)

    def down_ahead(way):
        up = both_sides(way, scattered_block(way, 0))
        for low in range(0, depth, tile):
            cols = slice(low, low + tile)
            part_sum = jnp.dot(up, w_down[:, cols], preferred_element_type=F32)
            own[way, 0, :, cols] = part_sum[:half]
            own[way, 1, :, cols] = part_sum[half:]

    def contribute_first(way):
        attended = attended_by(way, 0)
        for low in range(0, depth, tile):
            cols = slice(low, low + tile)
            part_sum = jnp.dot(attended, w_o[:, cols], preferred_element_type=F32)
            own[way, 0, :, cols] = own[way, 0, :, cols] + part_sum[:half]
            given[way, 0, :, cols] = (own[way, 1, :, cols] + part_sum[half:]).astype(BF16)

    def contribute(way, step):
        at = scattered_block(way, step)
        attended = attended_by(way, step)
        up = both_sides(way, at)

        @pl.when(step >= 2)
        def _():
            pair_copy(way, step - 2).wait_send()

        for low in range(0, depth, tile):
            cols = slice(low, low + tile)
            part_sum = (jnp.dot(attended, w_o[:, cols], preferred_element_type=F32)
                        + jnp.dot(up, w_down[:, cols], preferred_element_type=F32))
            own[way, step % 2, :, cols] = part_sum[:half]
            given[way, step % 2, :, cols] = part_sum[half:].astype(BF16)
        pair_copy(way, step).start()

    def total(way, step, part):
        span = span_of(part)
        taken = pl.ds(pl.multiple_of(half + part * piece, piece), piece)
        return own[way, step % 2, span] + hbuf[way, step, taken].astype(F32) + hbuf[way, step, span].astype(F32)

    def out_copy(way, part):
        span = pl.ds(way * half + part * piece, piece)
        return pltpu.make_async_copy(kept.at[span], out_hbm.at[span], edge_sem.at[1 + way * PARTS + part])

    def tell(phase):
        for to in (right, left, partner):
            pl.semaphore_signal(ready.at[phase], inc=1, device_id={"tp": to}, device_id_type=MESH)

    x_copy = pltpu.make_async_copy(x_hbm, kept, edge_sem.at[0])
    x_copy.start()
    def launch(layer, part, before_send):
        for way in range(2):
            low = way * half + part * piece
            hbuf[way, 0, pl.ds(pl.multiple_of(core * half + part * piece, piece), piece)] = layer_norm(
                kept[low:low + piece], gain[layer], bias[layer])
        before_send()
        for way in range(2):
            gather_copy(way, 0, part).start()
            share_copy(way, 0, part, core).start()

    barrier = call(right, left, partner)
    for copy in in_copies(0):
        copy.start()
    for g in range(3 * heads):
        staged[g, head_dim:] = jnp.zeros((LANES - head_dim, depth), BF16)
    for head in range(heads):
        w_o[head * LANES + head_dim:(head + 1) * LANES] = jnp.zeros((LANES - head_dim, depth), BF16)
    for wide, ref in ((b_up, bup_ref), (gain, gain_ref), (bias, bias_ref)):
        rows_f32 = ref[...].astype(F32)
        for layer in range(layers):
            wide[layer] = rows_f32[layer:layer + 1]
    rows_f32 = bo_ref[...].astype(F32) + bdown_ref[...].astype(F32)
    for layer in range(layers):
        b_sum[layer] = rows_f32[layer:layer + 1]
    column = lax.broadcasted_iota(jnp.int32, (1, 3 * width), 1)
    for layer in range(layers):
        b_qkv[layer] = jnp.where((column >= 2 * width) & (column % LANES == head_dim), 1.0, 0.0)
        for which, ref in enumerate((bq_ref, bk_ref, bv_ref)):
            heads_f32 = ref[layer].astype(F32)
            for head in range(heads):
                low = which * width + head * LANES
                b_qkv[layer, :, low:low + head_dim] = heads_f32[head:head + 1]
    x_copy.wait()
    pl.semaphore_wait(barrier, 3)
    for part in range(PARTS):
        launch(0, part, lambda: None)

    def layer_body(layer, carry):
        for copy in out_copies(layer):
            copy.start()

        @pl.when(layer == 0)
        def _():
            chips = lax.broadcasted_iota(jnp.int32, (RING, 1), 0) * (2 * rows)
            angle = chips.astype(F32) * freq_ref[...]
            cosine, sine = jnp.cos(angle), jnp.sin(angle)
            for at in range(RING):
                base_cos[at] = cosine[at:at + 1]
                base_sin[at] = sine[at:at + 1]
            row = lax.broadcasted_iota(jnp.int32, (rows, 1), 0)
            for way in range(2):
                offset = (row // half) * rows + way * half + row % half
                angle = offset.astype(F32) * freq_ref[...]
                step_cos[way] = jnp.cos(angle)
                step_sin[way] = jnp.sin(angle)

        for copy in in_copies(layer):
            copy.wait()
        for g in range(3 * heads):
            w_qkv[:, g * LANES:(g + 1) * LANES] = staged[g].T

        def arrive(event):
            step = 1 + event // 2
            for index in range(group):
                part = event % 2 * group + index
                for way in range(2):
                    gather_copy(way, step - 1, part).wait_recv()

                    @pl.when(step < RING - 1)
                    def _():
                        gather_copy(way, step, part).start()

                    share_copy(way, step, part, core).start()

        def first_units(unit, carry):
            project_kv(layer, unit, 0)
            project_rest(layer, unit, 0)
            return carry

        def events(event, carry):
            arrive(event)
            way, step = (event + 1) % 2, (event + 1) // 2
            project_kv(layer, way, step)
            project_rest(layer, way, step)

            @pl.when(event == 4)
            def _():
                for copy in out_copies(layer):
                    copy.wait()

            @pl.when((event >= 4) & (event < 6))
            def _():
                down_ahead(event - 4)

            @pl.when(event >= RING)
            def _():
                far, odd = (event - RING) // 2, event % 2
                attend_ahead((1 - odd) * (RING // 2 - far) + odd * (RING // 2 + far) * ((far + 1) // 2), 4)

            return carry

        def last_units(way, carry):
            project_kv(layer, way, RING - 1)
            return carry

        def nearest(side, carry):
            attend_ahead(1 + side * (RING - 2), 2)
            return carry

        for way in range(2):
            for slot in range(2):
                fresh(way, slot)
        lax.fori_loop(0, 2, first_units, 0)

        @pl.when(layer > 0)
        def _():
            pl.semaphore_wait(ready.at[4 * layer - 1], 3)

        arrive(0)
        lax.fori_loop(1, 2 * RING - 3, events, 0)
        attend_ahead(RING - 2, 4)
        arrive(2 * RING - 3)
        lax.fori_loop(0, 2, last_units, 0)

        def drain_gather(step, carry):
            for way in range(2):
                for part in range(PARTS):
                    @pl.when(step < RING - 1)
                    def _():
                        gather_copy(way, step, part).wait_send()

                    share_copy(way, step, part, core).wait_send()
            return carry

        lax.fori_loop(0, RING, drain_gather, 0)
        tell(4 * layer)
        lax.fori_loop(0, 2, nearest, 0)
        for way in range(2):
            hbuf[way, 0, :half] = jnp.zeros((half, depth), BF16)

        def first_parts(way, carry):
            contribute_first(way)

            @pl.when(way == 0)
            def _():
                pl.semaphore_wait(ready.at[4 * layer], 3)

            pair_copy(way, 0).start()
            return carry

        def scatter_events(event, carry):
            step, second = event // 2, event % 2

            @pl.when(event == 2 * RING - 4)
            def _():
                pl.semaphore_wait(ready.at[4 * layer + 1], 3)

            for index in range(group):
                part = second * group + index
                for way in range(2):
                    if index == 0:
                        @pl.when(second == 0)
                        def _():
                            pair_copy(way, step).wait_recv()

                    @pl.when(step > 0)
                    def _():
                        scatter_copy(way, step - 1, part).wait_recv()

                    hbuf[way, step, span_of(part)] = total(way, step, part).astype(BF16)
                    scatter_copy(way, step, part).start()
            contribute(second, step + 1)

            @pl.when((event >= 1) & (event < 3))
            def _():
                project_rest(layer, event - 1, RING - 1)

            @pl.when(event == 2)
            def _():
                tell(4 * layer + 1)

                @pl.when(layer < layers - 1)
                def _():
                    for copy in in_copies(layer + 1):
                        copy.start()

            return carry

        lax.fori_loop(0, 2, first_parts, 0)
        lax.fori_loop(0, 2 * RING - 2, scatter_events, 0)
        def drain_scatter(step, carry):
            for way in range(2):
                for part in range(PARTS):
                    scatter_copy(way, step, part).wait_send()
            return carry

        lax.fori_loop(0, 2, drain_scatter, 0)

        @pl.when(layer < layers - 1)
        def _():
            tell(4 * layer + 2)

        for part in range(PARTS):
            for way in range(2):
                if part == 0:
                    pair_copy(way, RING - 1).wait_recv()
                scatter_copy(way, RING - 2, part).wait_recv()
                low = way * half + part * piece
                hidden = kept[low:low + piece].astype(F32) + total(way, RING - 1, part) + b_sum[layer]
                kept[low:low + piece] = hidden.astype(BF16)

                @pl.when(layer == layers - 1)
                def _():
                    out_copy(way, part).start()

            @pl.when(layer < layers - 1)
            def _():
                def before_send():
                    if part == 0:
                        pl.semaphore_wait(ready.at[4 * layer + 2], 3)

                launch(layer + 1, part, before_send)

        lax.fori_loop(2, RING - 1, drain_scatter, 0)
        for way in range(2):
            for step in (RING - 2, RING - 1):
                pair_copy(way, step).wait_send()

        @pl.when(layer < layers - 1)
        def _():
            tell(4 * layer + 3)

        return carry

    lax.fori_loop(0, layers, layer_body, 0)
    for part in range(PARTS):
        for way in range(2):
            out_copy(way, part).wait()


def run_layers(x, w_q, w_k, w_v, w_o, w_up, w_down, vectors, freq):
    rows, depth = x.shape
    layers, heads, head_dim, _ = w_q.shape
    width, hidden_width = heads * LANES, w_up.shape[2]
    half = rows // 2
    vmem = pl.BlockSpec(memory_space=pltpu.VMEM)
    hbm = pl.BlockSpec(memory_space=pl.ANY)
    return pl.pallas_call(
        layers_kernel,
        out_shape=jax.ShapeDtypeStruct((rows, depth), BF16),
        in_specs=[hbm] * 7 + [vmem] * 9,
        out_specs=hbm,
        scratch_shapes=[
            pltpu.VMEM((rows, depth), BF16),
            pltpu.VMEM((RING, 1, LANES), F32),
            pltpu.VMEM((RING, 1, LANES), F32),
            pltpu.VMEM((2, rows, LANES), F32),
            pltpu.VMEM((2, rows, LANES), F32),
            pltpu.VMEM((layers, 1, 3 * width), F32),
            pltpu.VMEM((layers, 1, hidden_width), F32),
            pltpu.VMEM((layers, 1, depth), F32),
            pltpu.VMEM((layers, 1, depth), F32),
            pltpu.VMEM((layers, 1, depth), F32),
            pltpu.VMEM((2, RING, rows, depth), BF16),
            pltpu.VMEM((RING, 2, width, rows), BF16),
            pltpu.VMEM((RING, 2, rows, width), BF16),
            pltpu.VMEM((RING, 2, width, rows), BF16),
            pltpu.VMEM((RING, 2, rows, hidden_width), BF16),
            pltpu.VMEM((3 * heads, LANES, depth), BF16),
            pltpu.VMEM((depth, 3 * width), BF16),
            pltpu.VMEM((depth, hidden_width), BF16),
            pltpu.VMEM((width, depth), BF16),
            pltpu.VMEM((hidden_width, depth), BF16),
            pltpu.VMEM((2, 2, half, depth), BF16),
            pltpu.VMEM((2, 2, half, depth), F32),
            pltpu.VMEM((2, 2, heads, LANES, rows), F32),
            pltpu.VMEM((2, 2, heads, 1, rows), F32),
            pltpu.SemaphoreType.DMA((4 * heads + 2,)),
            pltpu.SemaphoreType.DMA((2, RING, PARTS)),
            pltpu.SemaphoreType.DMA((2, RING, PARTS)),
            pltpu.SemaphoreType.DMA((2, RING, PARTS)),
            pltpu.SemaphoreType.DMA((2, RING, PARTS)),
            pltpu.SemaphoreType.DMA((2, RING, PARTS)),
            pltpu.SemaphoreType.DMA((2, RING, PARTS)),
            pltpu.SemaphoreType.DMA((2, RING)),
            pltpu.SemaphoreType.DMA((2, RING)),
            pltpu.SemaphoreType.REGULAR((4 * layers,)),
            pltpu.SemaphoreType.DMA((1 + 2 * PARTS,)),
        ],
        compiler_params=pltpu.CompilerParams(collective_id=0, has_side_effects=True, vmem_limit_bytes=VMEM_LIMIT),
        name="layers",
    )(x, w_q, w_k, w_v, w_o, w_up, w_down, *vectors, freq)


def rotary_frequencies():
    lane = jnp.arange(LANES)
    pair = (lane % (ROT_DIM // 2)).astype(F32)
    return jnp.where(lane < ROT_DIM, 1.0 / (ROPE_BASE ** (pair * (2.0 / ROT_DIM))), 0.0).reshape(1, LANES)


def solution(mesh):
    head_spec = P(None, None, "tp", None)
    head_bias_spec = P(None, "tp", None)
    in_specs = (P("dp", "tp", None), P(), P(), head_spec, head_bias_spec, head_spec, head_bias_spec, head_spec, head_bias_spec,
                P(None, "tp", None, None), P(), P(None, None, "tp"), P(None, "tp"), P(None, "tp", None), P())

    def local_program(x_loc, ln_gain, ln_bias, w_q, b_q, w_k, b_k, w_v, b_v, w_o, b_o, w_up, b_up, w_down, b_down):
        def heads_first(weight):
            return jnp.transpose(weight, (0, 2, 3, 1))

        out = run_layers(x_loc[0], heads_first(w_q), heads_first(w_k), heads_first(w_v), w_o, w_up, w_down,
                         (b_q, b_k, b_v, b_up, b_o, b_down, ln_gain, ln_bias), rotary_frequencies())
        return out[None]

    return jax.shard_map(local_program, mesh=mesh, in_specs=in_specs, out_specs=P("dp", "tp", None), check_vma=False)
```
